512 devices in a mesh: gx: 4 (over y_hi, core), gy: 16 (over z), gz: 8 (over y_lo, x).
Axes of the slice: x: 4, y: 4 (y_hi: 2, y_lo: 2; y = y_hi * 2 + y_lo), z: 16, core: 2. Of those that a mesh axis runs over, the one named last changes fastest.
Arguments:
- heat_level_grid: float32 [256, 1024, 512], P('gz', 'gy', 'gx'), may hold values from -16 to 16, as said below
- interval_first_class: int32 [1], replicated, may hold values from 0 to 95
- interval_beyond_class: int32 [1], replicated, may hold values from 128 to 256
Outputs:
- magnitude: float32 [256, 1024, 512], P('gz', 'gy', 'gx')
- histogram: float32 [256], replicated
- stats: float32 [4], replicated
The draws below stay inside these ranges and needn't reach their ends.
Inputs may be any that keep to these rules, and one draw needn't show every extreme that they name: `heat_level_grid`: each entry is a rough value times an amplitude that is constant on blocks of 8 x 4 x 4 cells (z, y, x) and varies over a factor of 16 between blocks.
All inputs are finite; a program needn't handle non-finite values.
Results may differ from the reference program's by a relative error of at most 0.0003.
Values sent between devices are 32-bit elements; how exact they have to be, the bound alone decides.
A program may use at most 64 MiB of HBM per device.

```python
import math
import jax
import jax.numpy as jnp

BINS = 256
NX = 512
NY = 1024
NZ = 256


def draw_heat_level_grid(key, part):
    first_key, second_key = jax.random.split(jax.random.fold_in(key, 11))
    coarse = jax.random.uniform(first_key, (NZ // 8, NY // 4, NX // 4), jnp.float32, math.log(0.25), math.log(4.0))
    amplitude = jnp.exp(coarse)
    amplitude = jnp.repeat(jnp.repeat(jnp.repeat(amplitude, 8, axis=0), 4, axis=1), 4, axis=2)
    noise = jnp.clip(jax.random.normal(second_key, (NZ, NY, NX), jnp.float32), -4.0, 4.0)
    return (amplitude * noise).astype(jnp.float32)


def setup_inputs(seed: int = 0) -> dict:
    key_list = jax.random.split(jax.random.key(seed), 4)
    return {
        "heat_level_grid": draw_heat_level_grid(jax.random.fold_in(key_list[3], 71), 0),
        "interval_first_class": jax.random.randint(key_list[1], (1,), 0, 96).astype(jnp.int32),
        "interval_beyond_class": jax.random.randint(key_list[2], (1,), 128, BINS + 1).astype(jnp.int32),
    }


stencil_coefficients = (0.8, -0.2, 4.0 / 105.0, -1.0 / 280.0)
grad_range = 12.0

def directional_rate(field, direction_length_count):
    running = jnp.zeros_like(field)
    for offset, coefficient in enumerate(stencil_coefficients, start=1):
        running = running + coefficient * (jnp.roll(field, -offset, direction_length_count) - jnp.roll(field, offset, direction_length_count))
    return running

def reference(heat_level_grid, interval_first_class, interval_beyond_class):
    slope_norm_square = jnp.zeros_like(heat_level_grid)
    for direction_length_count in range(3):
        slope_in_direction = directional_rate(heat_level_grid, direction_length_count)
        slope_norm_square = slope_norm_square + slope_in_direction * slope_in_direction
    magnitude = jnp.sqrt(slope_norm_square + 1.0) - 1.0
    position = jnp.clip(magnitude * (BINS / grad_range), 0.5, BINS - 0.5)
    low_bin = jnp.minimum(jnp.floor(position - 0.5), BINS - 2).astype(jnp.int32)
    fraction = position - 0.5 - low_bin.astype(position.dtype)
    flat_low = low_bin.ravel()
    flat_frac = fraction.ravel()
    counts = jax.ops.segment_sum(1.0 - flat_frac, flat_low, BINS) + jax.ops.segment_sum(flat_frac, flat_low + 1, BINS)
    total_cells = NX * NY * NZ
    histogram = counts * (BINS / total_cells)
    lower_edge = interval_first_class[0]
    upper_edge = interval_beyond_class[0]
    high_bin = low_bin + 1
    inside_low = (low_bin >= lower_edge) & (low_bin < upper_edge)
    inside_high = (high_bin >= lower_edge) & (high_bin < upper_edge)
    weight = jnp.where(inside_low, 1.0 - fraction, 0.0) + jnp.where(inside_high, fraction, 0.0)
    lowest = jnp.min(magnitude + grad_range * (1.0 - weight))
    highest = jnp.max(weight * magnitude)
    weighted_sum = jnp.sum(weight * magnitude) / total_cells
    weighted_count = jnp.sum(weight) / total_cells
    stats = jnp.stack([lowest, highest, weighted_sum, weighted_count])
    return (magnitude, histogram, stats)
```

```python
import functools

import jax
import jax.numpy as jnp
from jax import lax
from jax.experimental import pallas as pl
from jax.experimental.pallas import tpu as pltpu
from jax.sharding import PartitionSpec as P

BINS = 256
FINE = 32
COARSE = BINS // FINE
GROUPS = 8
RANGE = 12.0
COEFS = (0.8, -0.2, 4.0 / 105.0, -1.0 / 280.0)
SCALE = 840.0
TAPS = (672.0, -168.0, 32.0, -3.0)
MESH = pl.DeviceIdType.MESH
F32 = jnp.float32
BF16 = jnp.bfloat16
UNROLL = 8
EDGE = 4


def tap(distance):
    value = jnp.zeros(distance.shape, F32)
    for k, t in enumerate(TAPS, start=1):
        value = jnp.where(distance == k, t, value)
        value = jnp.where(distance == -k, -t, value)
    return value


def kernel(
    sizes,
    first_ref,
    beyond_ref,
    x_ref,
    mag_ref,
    hist_ref,
    stat_ref,
    ext,
    packed,
    from_left,
    from_right,
    band,
    rim_band,
    rim_part,
    acc,
    gather_near,
    gather_far,
    in_sem,
    send_sem,
    recv_sem,
    ready_y,
    ready_z,
    all_send,
    all_recv,
):
    names = ("gx", "gy", "gz")
    nz, ny, nx = x_ref.shape
    where = {a: lax.axis_index(a) for a in names}
    near_total = sizes["gx"] * sizes["gz"]
    far_total = sizes["gy"]
    total = near_total * far_total

    loads = [
        pltpu.make_async_copy(
            x_ref.at[pl.ds(a, b)], ext.at[pl.ds(4 + a, b), pl.ds(8, ny)], in_sem.at[i]
        )
        for i, (a, b) in enumerate(((0, nz // 2), (nz // 2, nz - nz // 2)))
    ]
    for c in loads:
        c.start()

    ahead = {(a, d): lax.rem(where[a] + d, sizes[a]) for a in names for d in range(sizes[a])}

    def signal(sem, axis, distance):
        steps = sorted({distance % sizes[axis], -distance % sizes[axis]} - {0})
        for d in steps:
            pl.semaphore_signal(sem, inc=1, device_id={axis: ahead[axis, d]}, device_id_type=MESH)
        return len(steps)

    barrier = pltpu.get_barrier_semaphore()
    greeted = 0
    for d in range(1, sizes["gx"] // 2 + 1):
        greeted += signal(barrier, "gx", d)
    greeted += signal(barrier, "gz", 1)
    greeted += signal(barrier, "gy", 1)
    z_hops = [1 << i for i in range(max(1, (sizes["gz"] // 2).bit_length()))]
    y_hops = [1 << i for i in range(max(1, (sizes["gy"] // 4).bit_length()))]
    heard = {}

    def tell(axis, sems, hops, i):
        if i < len(hops):
            heard[axis, i] = signal(sems.at[i], axis, hops[i])

    def hear(axis, sems, hops, i):
        if i < len(hops):
            pl.semaphore_wait(sems.at[i], heard[axis, i])

    row = lax.broadcasted_iota(jnp.int32, (128, 128), 0)
    col = lax.broadcasted_iota(jnp.int32, (128, 128), 1)
    diag = tap(row - col).astype(BF16)
    band[0:128, :] = diag
    band[128:256, :] = diag
    r16 = lax.broadcasted_iota(jnp.int32, (16, 128), 0)
    l16 = lax.broadcasted_iota(jnp.int32, (16, 128), 1)
    m16 = lax.rem(r16, 8)
    place = jnp.where(m16 < 4, m16 - 4, 124 + m16)
    rim_tap = tap(place - l16)
    even = jnp.where(r16 < 8, rim_tap, 0.0).astype(BF16)
    odd = jnp.where(r16 >= 8, rim_tap, 0.0).astype(BF16)
    rim_band[...] = jnp.zeros(rim_band.shape, BF16)
    for j in range(16):
        tile = odd if j % 2 else even
        base = (j // 2) * 16
        rim_band[base : base + 16, 128 * j : 128 * (j + 1)] = tile
        rim_band[128 + base : 144 + base, 128 * j : 128 * (j + 1)] = tile
    acc[...] = jnp.zeros(acc.shape, F32)

    for c in loads:
        c.wait()

    planes = nz // 16
    lane = lax.broadcasted_iota(jnp.int32, (128, 128), 1)
    rims = None
    for j in range(16):
        block = ext[4 + planes * j : 4 + planes * (j + 1), 8 : 8 + ny, :].reshape(planes * ny, 128)
        turned = pltpu.roll(block, (8 * j + 4) % 128, 1)
        rims = turned if rims is None else jnp.where(lane >= 8 * j, turned, rims)
    packed[...] = rims

    pl.semaphore_wait(barrier, greeted)

    def up(a):
        return {a: lax.rem(where[a] + 1, sizes[a])}

    def down(a):
        return {a: lax.rem(where[a] + sizes[a] - 1, sizes[a])}

    def remote(src, dst, i, device):
        return pltpu.make_async_remote_copy(
            src_ref=src,
            dst_ref=dst,
            send_sem=send_sem.at[i],
            recv_sem=recv_sem.at[i],
            device_id=device,
            device_id_type=MESH,
        )

    own = pl.ds(4, nz)
    wide = pl.ds(8, ny)
    z_low = remote(ext.at[pl.ds(nz, 4), wide], ext.at[pl.ds(0, 4), wide], 4, up("gz"))
    z_high = remote(ext.at[pl.ds(4, 4), wide], ext.at[pl.ds(nz + 4, 4), wide], 5, down("gz"))
    y_low = remote(ext.at[own, pl.ds(4 + ny, 4)], ext.at[own, pl.ds(4, 4)], 2, up("gy"))
    y_high = remote(ext.at[own, pl.ds(8, 4)], ext.at[own, pl.ds(8 + ny, 4)], 3, down("gy"))
    x_low = remote(packed, from_left, 0, up("gx"))
    x_high = remote(packed, from_right, 1, down("gx"))
    x_low.start()
    x_high.start()
    y_low.start()
    y_high.start()
    z_low.start()
    z_high.start()
    tell("gz", ready_z, z_hops, 0)
    tell("gy", ready_y, y_hops, 0)

    x_low.wait()
    x_high.wait()
    rim = jnp.where(lax.rem(lane, 8) < 4, from_left[...], from_right[...])
    rim_hi = rim.astype(BF16)
    rim_lo = (rim - rim_hi.astype(F32)).astype(BF16)
    rim_part[...] = jnp.dot(
        jnp.concatenate([rim_hi, rim_lo], axis=1), rim_band[...], preferred_element_type=F32
    )
    lower = first_ref[0].astype(F32) - 1.0
    upper = beyond_ref[0].astype(F32)
    parity = jnp.where(lax.broadcasted_iota(jnp.int32, (16, 128), 0) >= 8, 1.0, 0.0)

    def twice(a):
        return jnp.concatenate([a, a], axis=0)

    def rates(blocks):
        sides = []
        for z, t0, nt in blocks:
            here = ext[z + 4, 8 + 8 * t0 : 8 + 8 * (t0 + nt), :]
            hi = here.astype(BF16)
            lo = (here - hi.astype(F32)).astype(BF16)
            sides.append(jnp.concatenate([hi, lo], axis=1))
        return jnp.dot(jnp.concatenate(sides, axis=0), band[...], preferred_element_type=F32)

    def plane(z, t0, nt, gx):
        y0, n = 8 + 8 * t0, 8 * nt
        rows = pl.multiple_of(lax.rem(z, planes) * ny + 8 * t0, 8)
        cols = pl.multiple_of((z // planes) * 128, 128)
        gx = (gx + rim_part[pl.ds(rows, n), pl.ds(cols, 128)]) * (1.0 / SCALE)
        gy = None
        gz = None
        for k, c in enumerate(COEFS, start=1):
            y_term = c * (ext[z + 4, y0 + k : y0 + k + n, :] - ext[z + 4, y0 - k : y0 - k + n, :])
            z_term = c * (ext[z + 4 + k, y0 : y0 + n, :] - ext[z + 4 - k, y0 : y0 + n, :])
            gy = y_term if gy is None else gy + y_term
            gz = z_term if gz is None else gz + z_term
        m = jnp.sqrt(gz * gz + gy * gy + gx * gx + 1.0) - 1.0
        mag_ref[z, 8 * t0 : 8 * (t0 + nt), :] = m
        q = jnp.clip(m * (BINS / RANGE), 0.5, BINS - 0.5) - 0.5
        low = jnp.minimum(jnp.floor(q), BINS - 2.0)
        frac = q - low
        w = jnp.clip(jnp.minimum(q - lower, upper - q), 0.0, 1.0)
        wm = w * m
        worst = m + RANGE * (1.0 - w)
        coarse = jnp.floor(low * (1.0 / FINE))
        fine = low - FINE * coarse
        frac_hi = frac.astype(BF16).astype(F32)
        frac_lo = frac - frac_hi
        left, right = [], []
        zero = jnp.zeros((16, 128), BF16)
        one = jnp.ones((16, 128), BF16)
        for i in range(nt):
            s = slice(8 * i, 8 * i + 8)
            c2 = (twice(coarse[s]) - parity).astype(BF16)
            f2 = (twice(fine[s]) - parity).astype(BF16)
            h2 = twice(frac_hi[s]).astype(BF16)
            l2 = twice(frac_lo[s]).astype(BF16)
            ones, his, los = [], [], []
            for j in range(COARSE // 2):
                hit = c2 == jnp.asarray(2 * j, BF16)
                ones.append(jnp.where(hit, one, zero))
                his.append(jnp.where(hit, h2, zero))
                los.append(jnp.where(hit, l2, zero))
            left.append(jnp.concatenate(ones + his + los, axis=0))
            right.append(
                jnp.concatenate(
                    [jnp.where(f2 == jnp.asarray(2 * j, BF16), one, zero) for j in range(FINE // 2)], axis=0
                )
            )
        fold = lambda op, a: functools.reduce(op, [a[8 * i : 8 * i + 8] for i in range(nt)])
        return left, right, fold(jnp.add, wm), fold(jnp.add, w), fold(jnp.maximum, wm), fold(jnp.minimum, worst)

    def several(blocks, carry):
        left, right = [], []
        s, n, hi, lo = carry
        gx = rates(blocks)
        start = 0
        for z, t0, nt in blocks:
            l, r, ps, pn, phi, plo = plane(z, t0, nt, gx[start : start + 8 * nt])
            start += 8 * nt
            left += l
            right += r
            s, n, hi, lo = s + ps, n + pn, jnp.maximum(hi, phi), jnp.minimum(lo, plo)
        acc[...] += lax.dot_general(
            jnp.concatenate(left, axis=1),
            jnp.concatenate(right, axis=1),
            (((1,), (1,)), ((), ())),
            preferred_element_type=F32,
        )
        return s, n, hi, lo

    zeros = jnp.zeros((8, 128), F32)
    carry = (zeros, zeros, zeros, jnp.full((8, 128), 3.0e38, F32))
    tiles = ny // 8
    inner = (nz - 8) // UNROLL
    carry = lax.fori_loop(
        0, inner, lambda t, c: several([(4 + t * UNROLL + u, 1, tiles - 2) for u in range(UNROLL)], c), carry
    )
    y_low.wait()
    y_high.wait()
    hear("gz", ready_z, z_hops, 0)
    hear("gy", ready_y, y_hops, 0)
    tell("gz", ready_z, z_hops, 1)
    tell("gy", ready_y, y_hops, 1)
    ends = [(u, t0, 1) for u in range(nz - 8) for t0 in (0, tiles - 1)]
    carry = lax.fori_loop(
        0, 1, lambda t, c: several([(4 + t * (nz - 8) + u, a, b) for u, a, b in ends], c), carry
    )
    z_low.wait()
    z_high.wait()
    hear("gz", ready_z, z_hops, 1)
    hear("gy", ready_y, y_hops, 1)
    tell("gz", ready_z, z_hops, 2)
    tell("gy", ready_y, y_hops, 2)

    def edge(t, c):
        z = t * EDGE
        z = z + (z // 4) * (nz - 8)
        return several([(z + u, 0, tiles) for u in range(EDGE)], c)

    wsum, wcount, highest, lowest = lax.fori_loop(0, 8 // EDGE, edge, carry)

    span = COARSE * GROUPS
    rows = lax.broadcasted_iota(jnp.int32, (span, FINE * GROUPS), 0)
    cols = lax.broadcasted_iota(jnp.int32, (span, FINE * GROUPS), 1)
    keep = lax.rem(rows, GROUPS) == lax.rem(cols, GROUPS)

    def by_class(a):
        a = jnp.where(keep, a, 0.0)
        return jnp.sum(a.reshape(COARSE, GROUPS, FINE * GROUPS), axis=1)

    count = by_class(acc[0:span, :])
    part = by_class(acc[span : 2 * span, :] + acc[2 * span : 3 * span, :])
    from_row = lax.broadcasted_iota(jnp.int32, (FINE * GROUPS, 128), 0) // GROUPS
    to_lane = lax.rem(lax.broadcasted_iota(jnp.int32, (FINE * GROUPS, 128), 1), FINE)
    spread = jnp.where(from_row == to_lane, 1.0, 0.0)
    both = jnp.dot(
        jnp.concatenate([count, part], axis=0),
        spread,
        precision=lax.Precision.HIGHEST,
        preferred_element_type=F32,
    )
    r8 = lax.broadcasted_iota(jnp.int32, (16, 128), 0)
    l8 = lax.broadcasted_iota(jnp.int32, (16, 128), 1)
    both = jnp.where(lax.rem(r8, 4) == l8 // FINE, both, 0.0)
    quad = [jnp.sum(both[4 * i : 4 * i + 4], axis=0, keepdims=True) for i in range(4)]
    lane1 = lax.broadcasted_iota(jnp.int32, (1, 128), 1)
    turned = [pltpu.roll(quad[2], 1, 1), pltpu.roll(quad[3], 1, 1)]
    row0 = quad[0] - quad[2] + jnp.where(lane1 == 0, turned[1], turned[0])
    row1 = quad[1] - quad[3] + jnp.where(lane1 == 0, turned[0], turned[1])

    def all_of(op, a):
        return op(op(a, axis=0, keepdims=True), axis=1, keepdims=True)

    row2 = jnp.where(
        lane1 == 0,
        all_of(jnp.min, lowest),
        jnp.where(
            lane1 == 1,
            all_of(jnp.max, highest),
            jnp.where(lane1 == 2, all_of(jnp.sum, wsum), all_of(jnp.sum, wcount)),
        ),
    )
    near = where["gx"] * sizes["gz"] + where["gz"]
    far = where["gy"]
    by_distance = lambda n: sorted(range(n), key=lambda d: -min(d, n - d))

    def share(buffer, slot, row, devices, i):
        buffer[slot] = row
        for device in devices:
            pltpu.make_async_remote_copy(
                src_ref=buffer.at[slot],
                dst_ref=buffer.at[slot],
                send_sem=all_send.at[i],
                recv_sem=all_recv.at[i],
                device_id=device,
                device_id_type=MESH,
            ).start()
        rest = buffer.at[pl.ds(0, len(devices))]
        pltpu.make_async_remote_copy(
            src_ref=rest,
            dst_ref=rest,
            send_sem=all_send.at[i],
            recv_sem=all_recv.at[i],
            device_id=up("gx"),
            device_id_type=MESH,
        ).wait()
        parts = buffer[...]
        summed = jnp.sum(parts, axis=0)
        smallest = jnp.min(parts[:, 2:3], axis=0)
        largest = jnp.max(parts[:, 2:3], axis=0)
        stat = jnp.where(lane1 == 0, smallest, jnp.where(lane1 == 1, largest, summed[2:3]))
        return jnp.concatenate([summed[0:2], stat, jnp.zeros((1, 128), F32)], axis=0)

    hear("gz", ready_z, z_hops, 2)
    row = jnp.concatenate([row0, row1, row2, jnp.zeros((1, 128), F32)], axis=0)
    row = share(
        gather_near,
        near,
        row,
        [
            {"gx": ahead["gx", dx], "gz": ahead["gz", dz]}
            for dz in by_distance(sizes["gz"])
            for dx in by_distance(sizes["gx"])
            if dx or dz
        ],
        0,
    )
    hear("gy", ready_y, y_hops, 2)
    row = share(
        gather_far, far, row, [{"gy": ahead["gy", dy]} for dy in by_distance(sizes["gy"]) if dy], 1
    )
    cells = nz * ny * nx * total
    hist_ref[...] = row[0:2] * (BINS / cells)
    stat_ref[...] = jnp.where(lane1 < 2, row[2:3], row[2:3] * (1.0 / cells))[:, 0:4]


def finish(mag_ref, hist_ref, stat_ref, mag_out, hist_out, stat_out, sem):
    copy = pltpu.make_async_copy(mag_ref, mag_out, sem)
    copy.start()
    hist_out[...] = hist_ref[...]
    stat_out[...] = stat_ref[...]
    copy.wait()


def solution(mesh):
    sizes = dict(mesh.shape)
    def on_device(grid, first, beyond):
        nz, ny, nx = grid.shape
        vmem = pl.BlockSpec(memory_space=pltpu.VMEM)
        hbm = pl.BlockSpec(memory_space=pltpu.HBM)
        packed_rows = nz * ny // 16
        magnitude, histogram, stats = pl.pallas_call(
            functools.partial(kernel, sizes),
            out_shape=(
                jax.ShapeDtypeStruct(grid.shape, F32),
                jax.ShapeDtypeStruct((2, 128), F32),
                jax.ShapeDtypeStruct((1, 4), F32),
            ),
            in_specs=[pl.BlockSpec(memory_space=pltpu.SMEM), pl.BlockSpec(memory_space=pltpu.SMEM), hbm],
            out_specs=(vmem, vmem, vmem),
            scratch_shapes=[
                pltpu.VMEM((nz + 8, ny + 16, nx), F32),
                pltpu.VMEM((packed_rows, 128), F32),
                pltpu.VMEM((packed_rows, 128), F32),
                pltpu.VMEM((packed_rows, 128), F32),
                pltpu.VMEM((256, 128), BF16),
                pltpu.VMEM((256, 2048), BF16),
                pltpu.VMEM((packed_rows, 2048), F32),
                pltpu.VMEM((3 * COARSE * GROUPS, FINE * GROUPS), F32),
                pltpu.VMEM((sizes["gx"] * sizes["gz"], 4, 128), F32),
                pltpu.VMEM((sizes["gy"], 4, 128), F32),
                pltpu.SemaphoreType.DMA((2,)),
                pltpu.SemaphoreType.DMA((6,)),
                pltpu.SemaphoreType.DMA((6,)),
                pltpu.SemaphoreType.REGULAR((3,)),
                pltpu.SemaphoreType.REGULAR((3,)),
                pltpu.SemaphoreType.DMA((2,)),
                pltpu.SemaphoreType.DMA((2,)),
            ],
            compiler_params=pltpu.CompilerParams(
                collective_id=0, has_side_effects=True, vmem_limit_bytes=32768 * 1024
            ),
        )(first, beyond, grid)
        magnitude, histogram, stats = pl.pallas_call(
            finish,
            out_shape=(
                jax.ShapeDtypeStruct(grid.shape, F32),
                jax.ShapeDtypeStruct((2, 128), F32),
                jax.ShapeDtypeStruct((1, 4), F32),
            ),
            in_specs=[vmem, vmem, vmem],
            out_specs=(hbm, vmem, vmem),
            scratch_shapes=[pltpu.SemaphoreType.DMA],
            compiler_params=pltpu.CompilerParams(vmem_limit_bytes=4 * 1024 * 1024),
        )(magnitude, histogram, stats)
        return magnitude, histogram.reshape(BINS), stats.reshape(4)

    return jax.shard_map(
        on_device,
        mesh=mesh,
        in_specs=(P("gz", "gy", "gx"), P(), P()),
        out_specs=(P("gz", "gy", "gx"), P(), P()),
        check_vma=False,
    )
```

```python
import functools

import jax
import jax.numpy as jnp
from jax import lax
from jax.experimental import pallas as pl
from jax.experimental.pallas import tpu as pltpu
from jax.sharding import PartitionSpec as P

BINS = 256
FINE = 24
COARSE = 12
GROUPS = 8
RANGE = 12.0
COEFS = (0.8, -0.2, 4.0 / 105.0, -1.0 / 280.0)
SCALE = 840.0
TAPS = (672.0, -168.0, 32.0, -3.0)
MESH = pl.DeviceIdType.MESH
F32 = jnp.float32
BF16 = jnp.bfloat16
SPAN = COARSE * GROUPS
WIDTH = FINE * GROUPS
BIG = 3.0e38
VMEM_KIB = 32768
DOTS = 2
HALVES = 2


def tap(distance):
    value = jnp.zeros(distance.shape, F32)
    for k, t in enumerate(TAPS, start=1):
        value = jnp.where(distance == k, t, value)
        value = jnp.where(distance == -k, -t, value)
    return value


def iota(shape, axis):
    return lax.broadcasted_iota(jnp.int32, shape, axis)


def kernel(
    sizes,
    first_ref,
    beyond_ref,
    x_ref,
    mag_ref,
    hist_ref,
    stat_ref,
    ext,
    packed,
    to_right,
    to_left,
    from_left,
    from_right,
    cross,
    rim_m,
    slope,
    square,
    rim_slope,
    rim_square,
    acc,
    unit,
    gather_near,
    gather_far,
    in_sem,
    send_sem,
    recv_sem,
    ready_y,
    ready_z,
    all_send,
    all_recv,
):
    names = ("gx", "gy", "gz")
    nz, ny, nx = x_ref.shape
    tiles = ny // 8
    where = {a: lax.axis_index(a) for a in names}
    total = sizes["gx"] * sizes["gy"] * sizes["gz"]
    ahead = {(a, d): lax.rem(where[a] + d, sizes[a]) for a in names for d in range(sizes[a])}

    loads = [
        pltpu.make_async_copy(
            x_ref.at[pl.ds(a, b - a)], ext.at[pl.ds(4 + a, b - a), pl.ds(8, ny)], in_sem.at[i]
        )
        for i, (a, b) in enumerate(((0, nz // 2), (nz // 2, nz)))
    ]
    for c in loads:
        c.start()

    def signal(sem, axis, distance):
        steps = sorted({distance % sizes[axis], -distance % sizes[axis]} - {0})
        for d in steps:
            pl.semaphore_signal(sem, inc=1, device_id={axis: ahead[axis, d]}, device_id_type=MESH)
        return len(steps)

    barrier = pltpu.get_barrier_semaphore()
    greeted = 0
    for d in range(1, sizes["gx"] // 2 + 1):
        greeted += signal(barrier, "gx", d)
    greeted += signal(barrier, "gz", 1)
    greeted += signal(barrier, "gy", 1)
    z_hops = [1 << i for i in range(max(1, (sizes["gz"] // 2).bit_length()))]
    y_hops = [1 << i for i in range(max(1, (sizes["gy"] // 4).bit_length()))]
    heard = {}

    def tell(axis, sems, hops, i):
        if i < len(hops):
            heard[axis, i] = signal(sems.at[i], axis, hops[i])

    def hear(axis, sems, hops, i):
        if i < len(hops):
            pl.semaphore_wait(sems.at[i], heard[axis, i])

    def up(a):
        return {a: ahead[a, 1]}

    def down(a):
        return {a: ahead[a, sizes[a] - 1]}

    def remote(src, dst, i, device):
        return pltpu.make_async_remote_copy(
            src_ref=src,
            dst_ref=dst,
            send_sem=send_sem.at[i],
            recv_sem=recv_sem.at[i],
            device_id=device,
            device_id_type=MESH,
        )

    own = pl.ds(4, nz)
    wide = pl.ds(8, ny)

    def z_pair(low, high, i):
        return (
            remote(ext.at[pl.ds(nz + low, 2), wide], ext.at[pl.ds(low, 2), wide], i, up("gz")),
            remote(ext.at[pl.ds(high, 2), wide], ext.at[pl.ds(nz + high, 2), wide], i + 1, down("gz")),
        )

    z_near = z_pair(2, 4, 4)
    z_far = z_pair(0, 6, 6)
    y_low = remote(ext.at[own, pl.ds(4 + ny, 4)], ext.at[own, pl.ds(4, 4)], 2, up("gy"))
    y_high = remote(ext.at[own, pl.ds(8, 4)], ext.at[own, pl.ds(8 + ny, 4)], 3, down("gy"))
    x_low = remote(to_right, from_left, 0, up("gx"))
    x_high = remote(to_left, from_right, 1, down("gx"))

    planes = 2
    rows = planes * ny
    half = rows // 2
    lane = iota((8, 128), 1)
    outer = jnp.logical_or(lane < 4, lane >= nx - 4)
    low_four = lax.rem(iota((half, 128), 1), 8) < 4

    def turn(a, j):
        return pltpu.roll(a, (8 * j + 4) % 128, 1)

    def back(a, j):
        return pltpu.roll(a, (124 - 8 * j) % 128, 1)

    gathered = [None] * (planes * tiles)
    for n, c in enumerate(loads):
        c.wait()
        groups = nz // planes // len(loads)
        for i in range(planes * tiles):
            u, t = i // tiles, i % tiles
            for j in range(n * groups, (n + 1) * groups):
                turned = turn(ext[4 + planes * j + u, 8 + 8 * t : 16 + 8 * t, :], j)
                gathered[i] = turned if j == 0 else jnp.where(lane >= 8 * j, turned, gathered[i])
    for i in range(planes * tiles):
        packed[8 * i : 8 * i + 8, :] = gathered[i]
    upper_half, lower_half = packed[0:half, :], packed[half:rows, :]
    to_right[...] = jnp.where(low_four, upper_half, pltpu.roll(lower_half, 4, 1))
    to_left[...] = jnp.where(low_four, pltpu.roll(upper_half, 124, 1), lower_half)

    pl.semaphore_wait(barrier, greeted)
    x_low.start()
    x_high.start()
    y_low.start()
    y_high.start()
    tell("gz", ready_z, z_hops, 0)
    tell("gy", ready_y, y_hops, 0)

    from_step = iota((WIDTH, BINS), 0) // GROUPS
    bin_of = iota((WIDTH, BINS), 1)
    digit = jnp.floor((bin_of.astype(F32) + 0.5) * (1.0 / FINE)).astype(jnp.int32)
    to_step = bin_of - FINE * digit
    single = jnp.where(to_step == FINE - 1, 1.0, 2.0)
    mix = jnp.where(from_step == to_step, single, jnp.where(jnp.abs(from_step - to_step) == 1, -1.0, 0.0))
    const = jnp.where(to_step == 0, 0.0, jnp.where(lax.rem(to_step, 2) == 1, -single, 2.0))
    r, c = iota((128, 128), 0), iota((128, 128), 1)
    same = jnp.logical_and(r // 8 == c // 8, (lax.rem(r, 8) < 4) != (lax.rem(c, 8) < 4))
    taps = jnp.where(same, tap(r - c), 0.0).astype(BF16)
    cross[...] = jnp.concatenate([taps, taps], axis=0)
    unit[...] = jnp.where(from_step == 0, const, mix).astype(BF16)
    for c in (*z_near, *z_far):
        c.start()

    lower = first_ref[...].astype(F32) - 1.0
    upper = beyond_ref[...].astype(F32)
    parity = jnp.where(iota((16, 128), 0) >= 8, 1.0, 0.0)
    lane16 = iota((16, 128), 1)
    never = jnp.full((16, 128), 1024.0, F32)
    inner_parity = jnp.where(jnp.logical_or(lane16 < 4, lane16 >= nx - 4), never, parity).astype(BF16)
    parity = parity.astype(BF16)
    zero = jnp.zeros((16, 128), BF16)
    one = jnp.ones((16, 128), BF16)

    def twice(a):
        return jnp.concatenate([a, a], axis=0).astype(BF16)

    def rates(z, t):
        y = 8 + 8 * t
        here = ext[z + 4, y : y + 8, :]
        gx = gy = gz = None
        for k, c in enumerate(COEFS, start=1):
            x_term = c * (pltpu.roll(here, 128 - k, 1) - pltpu.roll(here, k, 1))
            y_term = c * (ext[z + 4, y + k : y + k + 8, :] - ext[z + 4, y - k : y - k + 8, :])
            z_term = c * (ext[z + 4 + k, y : y + 8, :] - ext[z + 4 - k, y : y + 8, :])
            gx = x_term if gx is None else gx + x_term
            gy = y_term if gy is None else gy + y_term
            gz = z_term if gz is None else gz + z_term
        return gx, gy * gy + gz * gz

    def length(gx, rest):
        s = (rest + gx * gx) + 1.0
        return s * lax.rsqrt(s) - 1.0

    def classes(m, offset):
        q = jnp.clip(m * (BINS / RANGE) - 0.5, 0.0, BINS - 1.0)
        low = jnp.minimum(jnp.floor(q), BINS - 2.0)
        w = jnp.clip(jnp.minimum(q - lower, upper - q), 0.0, 1.0)
        coarse = jnp.floor(low * (1.000001 / FINE))
        c2 = twice(coarse) - offset
        f2 = twice(low - FINE * coarse) - parity
        h2 = twice(q - low)
        ones, parts = [], []
        for j in range(COARSE // 2):
            hit = c2 == jnp.asarray(2 * j, BF16)
            ones.append(jnp.where(hit, one, zero))
            parts.append(jnp.where(hit, h2, zero))
        steps = [jnp.minimum(f2, parity - one)]
        steps += [jnp.minimum(f2, jnp.asarray(2 * j, BF16)) for j in range(1, FINE // 2)]
        wm = w * m
        stats = (wm, w, wm, m - RANGE * w)
        return jnp.concatenate(ones + parts, axis=0), jnp.concatenate(steps, axis=0), stats

    def merge(a, b):
        return (a[0] + b[0], a[1] + b[1], jnp.maximum(a[2], b[2]), jnp.minimum(a[3], b[3]))

    def tally_up(items, fresh=False):
        share_of = len(items) // 2
        for i in range(2):
            part = items[i * share_of : (i + 1) * share_of]
            left = jnp.concatenate([a for a, _, _ in part], axis=1)
            right = jnp.concatenate([b for _, b, _ in part], axis=1)
            product = lax.dot_general(left, right, (((1,), (1,)), ((), ())), preferred_element_type=F32)
            if fresh:
                acc[i] = product
            else:
                acc[i] += product
        return functools.reduce(merge, [s for _, _, s in items])

    def deferred(z, t):
        gx, rest = rates(z, t)
        at = (z, slice(8 * t, 8 * t + 8), slice(None))
        slope[at] = gx
        square[at] = rest
        m = length(gx, rest)
        mag_ref[at] = m
        return classes(m, inner_parity)

    def fold(groups, span):
        for i in [u * tiles + t for u in range(planes) for t in span]:
            u, t = i // tiles, i % tiles
            for whole, kept in ((slope, rim_slope), (square, rim_square)):
                out = None
                for first, last in groups:
                    run = None
                    for j in range(first, last):
                        turned = turn(whole[planes * j + u, 8 * t : 8 * t + 8, :], j)
                        run = turned if run is None else jnp.where(lane >= 8 * j, turned, run)
                    if len(groups) == 1:
                        out = run
                    elif out is None:
                        out = jnp.where(lane < 8 * last, run, kept[8 * i : 8 * i + 8, :])
                    else:
                        out = jnp.where(lane >= 8 * first, run, out)
                kept[8 * i : 8 * i + 8, :] = out

    inside = list(range(4, nz - 4))
    count = nz // planes
    inner = [tally_up([deferred(z, t) for z in inside for t in range(1, tiles - 1)], True)]
    fold([(2, count - 2)], range(1, tiles - 1))

    hear("gz", ready_z, z_hops, 0)
    hear("gy", ready_y, y_hops, 0)
    tell("gz", ready_z, z_hops, 1)
    tell("gy", ready_y, y_hops, 1)
    y_low.wait()
    y_high.wait()
    inner.append(tally_up([deferred(z, t) for z in inside for t in (0, tiles - 1)]))
    fold([(2, count - 2)], (0, tiles - 1))
    for c in z_near:
        c.wait()
    hear("gz", ready_z, z_hops, 1)
    hear("gy", ready_y, y_hops, 1)
    tell("gz", ready_z, z_hops, 2)
    tell("gy", ready_y, y_hops, 2)
    inner.append(tally_up([deferred(z, t) for z in (2, 3, nz - 4, nz - 3) for t in range(tiles)]))
    for c in z_far:
        c.wait()
    inner.append(tally_up([deferred(z, t) for z in (0, 1, nz - 2, nz - 1) for t in range(tiles)]))
    fold([(0, 2), (count - 2, count)], range(tiles))
    inner = functools.reduce(merge, inner)

    x_low.wait()
    x_high.wait()
    left_rim, right_rim = from_left[...], from_right[...]
    extra = (
        jnp.concatenate(
            [
                jnp.where(low_four, left_rim, pltpu.roll(right_rim, 4, 1)),
                jnp.where(low_four, pltpu.roll(left_rim, 124, 1), right_rim),
            ],
            axis=0,
        )
        - packed[...]
    )
    extra_hi = extra.astype(BF16)
    extra_lo = (extra - extra_hi.astype(F32)).astype(BF16)
    corr = jnp.dot(
        jnp.concatenate([extra_hi, extra_lo], axis=1), cross[...], preferred_element_type=F32
    ) * (1.0 / SCALE)
    rim = []
    for i in range(planes * tiles):
        at = slice(8 * i, 8 * i + 8)
        m = length(rim_slope[at, :] + corr[at], rim_square[at, :])
        rim_m[at, :] = m
        rim.append(classes(m, parity))
    rim = tally_up(rim)
    tally = acc[0] + acc[1]

    def only(keep, s):
        return (
            jnp.where(keep, s[0], 0.0),
            jnp.where(keep, s[1], 0.0),
            jnp.where(keep, s[2], 0.0),
            jnp.where(keep, s[3], BIG),
        )

    wsum, wcount, highest, lowest = functools.reduce(
        merge, [only(jnp.logical_not(outer), inner), rim]
    )

    keep = iota((GROUPS, WIDTH), 0) == lax.rem(iota((GROUPS, WIDTH), 1), GROUPS)

    def by_class(a):
        return jnp.sum(jnp.where(keep[None], a.reshape(COARSE, GROUPS, WIDTH), 0.0), axis=1)

    sums = jnp.concatenate([by_class(tally[0:SPAN, :]), by_class(tally[SPAN : 2 * SPAN, :])], axis=0)
    high = sums.astype(BF16)
    rest = sums - high.astype(F32)
    middle_bits = rest.astype(BF16)
    low_bits = (rest - middle_bits.astype(F32)).astype(BF16)
    three = jnp.dot(
        jnp.concatenate([high.astype(F32), middle_bits.astype(F32), low_bits.astype(F32)], axis=0).astype(BF16),
        unit[...],
        preferred_element_type=F32,
    )
    n = 2 * COARSE
    both = (three[2 * n : 3 * n] + three[n : 2 * n]) + three[0:n]
    place = iota((2 * COARSE, BINS), 1).astype(F32)
    digit = jnp.floor((place + 0.5) * (1.0 / FINE)).astype(jnp.int32)
    both = jnp.where(lax.rem(iota((2 * COARSE, BINS), 0), COARSE) == digit, both, 0.0)
    low_sum = jnp.sum(both[0:COARSE, :], axis=0, keepdims=True)
    part = jnp.sum(both[COARSE : 2 * COARSE, :], axis=0, keepdims=True)
    lane1 = iota((1, 128), 1)
    turned = [pltpu.roll(part[:, 0:128], 1, 1), pltpu.roll(part[:, 128:256], 1, 1)]
    row0 = low_sum[:, 0:128] - part[:, 0:128] + jnp.where(lane1 == 0, turned[1], turned[0])
    row1 = low_sum[:, 128:256] - part[:, 128:256] + jnp.where(lane1 == 0, turned[0], turned[1])

    def all_of(op, a):
        return op(op(a, axis=0, keepdims=True), axis=1, keepdims=True)

    row2 = jnp.where(
        lane1 == 0,
        all_of(jnp.min, lowest) + RANGE,
        jnp.where(
            lane1 == 1,
            all_of(jnp.max, highest),
            jnp.where(lane1 == 2, all_of(jnp.sum, wsum), all_of(jnp.sum, wcount)),
        ),
    )
    near = where["gx"] * sizes["gz"] + where["gz"]
    far = where["gy"]
    by_distance = lambda n: sorted(range(n), key=lambda d: -min(d, n - d))

    def share(buffer, slot, devices, i, meanwhile=lambda: None):
        for device in devices:
            pltpu.make_async_remote_copy(
                src_ref=buffer.at[slot],
                dst_ref=buffer.at[slot],
                send_sem=all_send.at[i],
                recv_sem=all_recv.at[i],
                device_id=device,
                device_id_type=MESH,
            ).start()
        others = buffer.at[pl.ds(0, len(devices))]
        arrival = pltpu.make_async_remote_copy(
            src_ref=others,
            dst_ref=others,
            send_sem=all_send.at[i],
            recv_sem=all_recv.at[i],
            device_id=up("gx"),
            device_id_type=MESH,
        )
        meanwhile()
        arrival.wait()
        parts = buffer[...]
        summed = jnp.sum(parts, axis=0)
        smallest = jnp.min(parts[:, 2:3], axis=0)
        largest = jnp.max(parts[:, 2:3], axis=0)
        stat = jnp.where(lane1 == 0, smallest, jnp.where(lane1 == 1, largest, summed[2:3]))
        return jnp.concatenate([summed[0:2], stat, jnp.zeros((1, 128), F32)], axis=0)

    def put_rims():
        for i in range(planes * tiles):
            u, t = i // tiles, i % tiles
            m = rim_m[8 * i : 8 * i + 8, :]
            for j in range(count):
                at = (planes * j + u, slice(8 * t, 8 * t + 8), slice(None))
                mag_ref[at] = jnp.where(outer, back(m, j), mag_ref[at])

    gather_near[near] = jnp.concatenate([row0, row1, row2, jnp.zeros((1, 128), F32)], axis=0)
    hear("gz", ready_z, z_hops, 2)
    row = share(
        gather_near,
        near,
        [
            {"gx": ahead["gx", dx], "gz": ahead["gz", dz]}
            for dz in by_distance(sizes["gz"])
            for dx in by_distance(sizes["gx"])
            if dx or dz
        ],
        0,
        put_rims,
    )
    gather_far[far] = row
    hear("gy", ready_y, y_hops, 2)
    row = share(gather_far, far, [{"gy": ahead["gy", dy]} for dy in by_distance(sizes["gy"]) if dy], 1)
    cells = nz * ny * nx * total
    hist_ref[...] = row[0:2] * (BINS / cells)
    stat_ref[...] = jnp.where(lane1 < 2, row[2:3], row[2:3] * (1.0 / cells))[:, 0:4]


def finish(mag_ref, hist_ref, stat_ref, mag_out, hist_out, stat_out, sem):
    copy = pltpu.make_async_copy(mag_ref, mag_out, sem)
    copy.start()
    hist_out[...] = hist_ref[...]
    stat_out[...] = stat_ref[...]
    copy.wait()


def solution(mesh):
    sizes = dict(mesh.shape)

    def on_device(grid, first, beyond):
        nz, ny, nx = grid.shape
        vmem = pl.BlockSpec(memory_space=pltpu.VMEM)
        hbm = pl.BlockSpec(memory_space=pltpu.HBM)
        results = (
            jax.ShapeDtypeStruct(grid.shape, F32),
            jax.ShapeDtypeStruct((2, 128), F32),
            jax.ShapeDtypeStruct((1, 4), F32),
        )
        magnitude, histogram, stats = pl.pallas_call(
            functools.partial(kernel, sizes),
            out_shape=results,
            in_specs=[vmem, vmem, hbm],
            out_specs=(vmem, vmem, vmem),
            scratch_shapes=[
                pltpu.VMEM((nz + 8, ny + 16, nx), F32),
                pltpu.VMEM((2 * ny, 128), F32),
                pltpu.VMEM((ny, 128), F32),
                pltpu.VMEM((ny, 128), F32),
                pltpu.VMEM((ny, 128), F32),
                pltpu.VMEM((ny, 128), F32),
                pltpu.VMEM((256, 128), BF16),
                pltpu.VMEM((2 * ny, 128), F32),
                pltpu.VMEM((nz, ny, nx), F32),
                pltpu.VMEM((nz, ny, nx), F32),
                pltpu.VMEM((2 * ny, 128), F32),
                pltpu.VMEM((2 * ny, 128), F32),
                pltpu.VMEM((2, 2 * SPAN, WIDTH), F32),
                pltpu.VMEM((WIDTH, BINS), BF16),
                pltpu.VMEM((sizes["gx"] * sizes["gz"], 4, 128), F32),
                pltpu.VMEM((sizes["gy"], 4, 128), F32),
                pltpu.SemaphoreType.DMA((2,)),
                pltpu.SemaphoreType.DMA((8,)),
                pltpu.SemaphoreType.DMA((8,)),
                pltpu.SemaphoreType.REGULAR((3,)),
                pltpu.SemaphoreType.REGULAR((3,)),
                pltpu.SemaphoreType.DMA((2,)),
                pltpu.SemaphoreType.DMA((2,)),
            ],
            compiler_params=pltpu.CompilerParams(
                collective_id=0, has_side_effects=True, vmem_limit_bytes=VMEM_KIB * 1024
            ),
        )(first.reshape(1, 1), beyond.reshape(1, 1), pltpu.with_memory_space_constraint(grid, pltpu.HBM))
        magnitude, histogram, stats = pl.pallas_call(
            finish,
            out_shape=results,
            in_specs=[vmem, vmem, vmem],
            out_specs=(hbm, vmem, vmem),
            scratch_shapes=[pltpu.SemaphoreType.DMA],
            compiler_params=pltpu.CompilerParams(vmem_limit_bytes=4 * 1024 * 1024),
        )(magnitude, histogram, stats)
        return magnitude, histogram.reshape(BINS), stats.reshape(4)

    return jax.shard_map(
        on_device,
        mesh=mesh,
        in_specs=(P("gz", "gy", "gx"), P(), P()),
        out_specs=(P("gz", "gy", "gx"), P(), P()),
        check_vma=False,
    )
```

```python
import functools

import jax
import jax.numpy as jnp
from jax import lax
from jax.experimental import pallas as pl
from jax.experimental.pallas import tpu as pltpu
from jax.sharding import PartitionSpec as P

BINS = 256
FINE = 24
COARSE = 12
GROUPS = 8
RANGE = 12.0
COEFS = (0.8, -0.2, 4.0 / 105.0, -1.0 / 280.0)
SCALE = 840.0
TAPS = (672.0, -168.0, 32.0, -3.0)
MESH = pl.DeviceIdType.MESH
F32 = jnp.float32
BF16 = jnp.bfloat16
SPAN = COARSE * GROUPS
WIDTH = FINE * GROUPS
BIG = 3.0e38
VMEM_KIB = 32768
DOTS = 2
HALVES = 2


def tap(distance):
    value = jnp.zeros(distance.shape, F32)
    for k, t in enumerate(TAPS, start=1):
        value = jnp.where(distance == k, t, value)
        value = jnp.where(distance == -k, -t, value)
    return value


def iota(shape, axis):
    return lax.broadcasted_iota(jnp.int32, shape, axis)


def kernel(
    sizes,
    first_ref,
    beyond_ref,
    x_ref,
    mag_ref,
    hist_ref,
    stat_ref,
    ext,
    packed,
    to_right,
    to_left,
    from_left,
    from_right,
    to_above,
    to_below,
    from_below,
    from_above,
    cross,
    rim_m,
    slope,
    square,
    rim_slope,
    rim_square,
    acc,
    unit,
    gather_near,
    gather_far,
    in_sem,
    send_sem,
    recv_sem,
    ready_y,
    ready_z,
    all_send,
    all_recv,
):
    names = ("gx", "gy", "gz")
    nz, ny, nx = x_ref.shape
    tiles = ny // 8
    where = {a: lax.axis_index(a) for a in names}
    total = sizes["gx"] * sizes["gy"] * sizes["gz"]
    ahead = {(a, d): lax.rem(where[a] + d, sizes[a]) for a in names for d in range(sizes[a])}

    loads = [
        pltpu.make_async_copy(
            x_ref.at[pl.ds(a, b - a)], ext.at[pl.ds(4 + a, b - a), pl.ds(8, ny)], in_sem.at[i]
        )
        for i, (a, b) in enumerate(((0, 4), (nz - 4, nz), (4, nz // 2), (nz // 2, nz - 4)))
    ]
    for c in loads:
        c.start()

    def signal(sem, axis, distances):
        n = sizes[axis]
        steps = sorted({step % n for d in distances for step in (d, -d)} - {0})
        for d in steps:
            pl.semaphore_signal(sem, inc=1, device_id={axis: ahead[axis, d]}, device_id_type=MESH)
        return len(steps)

    barrier = pltpu.get_barrier_semaphore()
    greeted = (
        signal(barrier, "gx", range(1, sizes["gx"]))
        + signal(barrier, "gz", (1, 2))
        + signal(barrier, "gy", (1, 2))
    )
    z_hops = ((1, 2), range(3, sizes["gz"] // 2 + 1))
    y_hops = ((2,), (4,))
    heard = {}

    def tell(axis, sems, hops, i):
        heard[axis, i] = signal(sems.at[i], axis, hops[i])

    def hear(axis, sems, i):
        if heard[axis, i]:
            pl.semaphore_wait(sems.at[i], heard[axis, i])

    def up(a):
        return {a: ahead[a, 1]}

    def down(a):
        return {a: ahead[a, sizes[a] - 1]}

    def remote(src, dst, i, device):
        return pltpu.make_async_remote_copy(
            src_ref=src,
            dst_ref=dst,
            send_sem=send_sem.at[i],
            recv_sem=recv_sem.at[i],
            device_id=device,
            device_id_type=MESH,
        )

    own = slice(4, 4 + nz)
    wide = pl.ds(8, ny)

    z_sends = (
        remote(ext.at[pl.ds(nz, 4), wide], ext.at[pl.ds(0, 4), wide], 4, up("gz")),
        remote(ext.at[pl.ds(4, 4), wide], ext.at[pl.ds(nz + 4, 4), wide], 5, down("gz")),
    )
    y_low = remote(to_above, from_below, 2, up("gy"))
    y_high = remote(to_below, from_above, 3, down("gy"))
    x_low = remote(to_right, from_left, 0, up("gx"))
    x_high = remote(to_left, from_right, 1, down("gx"))

    planes = 2
    rows = planes * ny
    half = rows // 2
    lane = iota((8, 128), 1)
    outer = jnp.logical_or(lane < 4, lane >= nx - 4)
    low_four = lax.rem(iota((half, 128), 1), 8) < 4

    def turn(a, j):
        return pltpu.roll(a, (8 * j + 4) % 128, 1)

    def back(a, j):
        return pltpu.roll(a, (124 - 8 * j) % 128, 1)

    loads[0].wait()
    loads[1].wait()
    pl.semaphore_wait(barrier, greeted)
    for c in z_sends:
        c.start()
    loads[2].wait()
    loads[3].wait()
    to_above[...] = ext[own, 4 + ny : 8 + ny, :]
    to_below[...] = ext[own, 8:12, :]
    y_low.start()
    y_high.start()
    tell("gz", ready_z, z_hops, 0)
    tell("gy", ready_y, y_hops, 0)

    from_step = iota((WIDTH, BINS), 0) // GROUPS
    bin_of = iota((WIDTH, BINS), 1)
    digit = jnp.floor((bin_of.astype(F32) + 0.5) * (1.0 / FINE)).astype(jnp.int32)
    to_step = bin_of - FINE * digit
    single = jnp.where(to_step == FINE - 1, 1.0, 2.0)
    mix = jnp.where(from_step == to_step, single, jnp.where(jnp.abs(from_step - to_step) == 1, -1.0, 0.0))
    const = jnp.where(to_step == 0, 0.0, jnp.where(lax.rem(to_step, 2) == 1, -single, 2.0))
    r, c = iota((128, 128), 0), iota((128, 128), 1)
    same = jnp.logical_and(r // 8 == c // 8, (lax.rem(r, 8) < 4) != (lax.rem(c, 8) < 4))
    taps = jnp.where(same, tap(r - c), 0.0).astype(BF16)
    cross[...] = jnp.concatenate([taps, taps], axis=0)
    unit[...] = jnp.where(from_step == 0, const, mix).astype(BF16)

    lower = first_ref[...].astype(F32) - 1.0
    upper = beyond_ref[...].astype(F32)
    parity = jnp.where(iota((16, 128), 0) >= 8, 1.0, 0.0)
    lane16 = iota((16, 128), 1)
    never = jnp.full((16, 128), 1024.0, F32)
    inner_parity = jnp.where(jnp.logical_or(lane16 < 4, lane16 >= nx - 4), never, parity).astype(BF16)
    parity = parity.astype(BF16)
    zero = jnp.zeros((16, 128), BF16)
    one = jnp.ones((16, 128), BF16)

    def twice(a):
        return jnp.concatenate([a, a], axis=0).astype(BF16)

    def slant(pairs):
        total_ = None
        for c, (ahead_, behind) in zip(COEFS, pairs):
            term = c * (ahead_ - behind)
            total_ = term if total_ is None else total_ + term
        return total_

    steps = range(1, len(COEFS) + 1)

    def along_x(z, t):
        here = ext[z + 4, 8 + 8 * t : 16 + 8 * t, :]
        return slant([(pltpu.roll(here, 128 - k, 1), pltpu.roll(here, k, 1)) for k in steps])

    def along_y(z, t):
        y = 8 + 8 * t
        g = slant([(ext[z + 4, y + k : y + k + 8, :], ext[z + 4, y - k : y - k + 8, :]) for k in steps])
        return g * g

    def along_z(z, t):
        y = slice(8 + 8 * t, 16 + 8 * t)
        g = slant([(ext[z + 4 + k, y, :], ext[z + 4 - k, y, :]) for k in steps])
        return g * g

    def length(gx, rest):
        s = (rest + gx * gx) + 1.0
        return s * lax.rsqrt(s) - 1.0

    def classes(m, offset):
        q = jnp.clip(m * (BINS / RANGE) - 0.5, 0.0, BINS - 1.0)
        low = jnp.minimum(jnp.floor(q), BINS - 2.0)
        w = jnp.clip(jnp.minimum(q - lower, upper - q), 0.0, 1.0)
        coarse = jnp.floor(low * (1.000001 / FINE))
        c2 = twice(coarse) - offset
        f2 = twice(low - FINE * coarse) - parity
        h2 = twice(q - low)
        ones, parts = [], []
        for j in range(COARSE // 2):
            hit = c2 == jnp.asarray(2 * j, BF16)
            ones.append(jnp.where(hit, one, zero))
            parts.append(jnp.where(hit, h2, zero))
        ladder = [jnp.minimum(f2, parity - one)]
        ladder += [jnp.minimum(f2, jnp.asarray(2 * j, BF16)) for j in range(1, FINE // 2)]
        wm = w * m
        stats = (wm, w, wm, m - RANGE * w)
        return jnp.concatenate(ones + parts, axis=0), jnp.concatenate(ladder, axis=0), stats

    def merge(a, b):
        return (a[0] + b[0], a[1] + b[1], jnp.maximum(a[2], b[2]), jnp.minimum(a[3], b[3]))

    def tally_up(items, fresh=False):
        share_of = len(items) // 2
        for i in range(2):
            part = items[i * share_of : (i + 1) * share_of]
            left = jnp.concatenate([a for a, _, _ in part], axis=1)
            right = jnp.concatenate([b for _, b, _ in part], axis=1)
            product = lax.dot_general(left, right, (((1,), (1,)), ((), ())), preferred_element_type=F32)
            if fresh:
                acc[i] = product
            else:
                acc[i] += product
        return functools.reduce(merge, [s for _, _, s in items])

    def place_of(z, t):
        return (z, slice(8 * t, 8 * t + 8), slice(None))

    def deferred(z, t, known=None, *parts):
        at = place_of(z, t)
        if known is None:
            gx, rest = along_x(z, t), None
            slope[at] = gx
        else:
            gx, rest = slope[at], square[at] if known else None
        for part in parts:
            g = part(z, t)
            rest = g if rest is None else rest + g
        square[at] = rest
        m = length(gx, rest)
        mag_ref[at] = m
        return classes(m, inner_parity)

    def prepare(z, t, part):
        at = place_of(z, t)
        slope[at] = along_x(z, t)
        if part is not None:
            square[at] = part(z, t)

    def fold(groups, span):
        for i in [u * tiles + t for u in range(planes) for t in span]:
            u, t = i // tiles, i % tiles
            for whole, kept in ((slope, rim_slope), (square, rim_square)):
                out = None
                for first, last in groups:
                    run = None
                    for j in range(first, last):
                        turned = turn(whole[planes * j + u, 8 * t : 8 * t + 8, :], j)
                        run = turned if run is None else jnp.where(lane >= 8 * j, turned, run)
                    if len(groups) == 1:
                        out = run
                    elif out is None:
                        out = jnp.where(lane < 8 * last, run, kept[8 * i : 8 * i + 8, :])
                    else:
                        out = jnp.where(lane >= 8 * first, run, out)
                kept[8 * i : 8 * i + 8, :] = out

    inside = list(range(4, nz - 4))
    count = nz // planes
    outside = [z for z in range(nz) if z not in inside]
    for t in range(tiles):
        edge_row = t in (0, tiles - 1)
        for z in inside if edge_row else ():
            prepare(z, t, along_z)
        for z in outside:
            prepare(z, t, None if edge_row else along_y)
    gathered = [None] * (planes * tiles)
    for i in range(planes * tiles):
        u, t = i // tiles, i % tiles
        for j in range(nz // planes):
            turned = turn(ext[4 + planes * j + u, 8 + 8 * t : 16 + 8 * t, :], j)
            gathered[i] = turned if j == 0 else jnp.where(lane >= 8 * j, turned, gathered[i])
        packed[8 * i : 8 * i + 8, :] = gathered[i]
    upper_half, lower_half = packed[0:half, :], packed[half:rows, :]
    to_right[...] = jnp.where(low_four, upper_half, pltpu.roll(lower_half, 4, 1))
    to_left[...] = jnp.where(low_four, pltpu.roll(upper_half, 124, 1), lower_half)
    x_low.start()
    x_high.start()

    inner = [
        tally_up([deferred(z, t, None, along_y, along_z) for z in inside for t in range(1, tiles - 1)], True)
    ]
    fold([(2, count - 2)], range(1, tiles - 1))

    hear("gz", ready_z, 0)
    hear("gy", ready_y, 0)
    tell("gz", ready_z, z_hops, 1)
    tell("gy", ready_y, y_hops, 1)
    y_low.wait()
    y_high.wait()
    ext[own, 4:8, :] = from_below[...]
    ext[own, 8 + ny : 12 + ny, :] = from_above[...]
    inner.append(tally_up([deferred(z, t, True, along_y) for z in inside for t in (0, tiles - 1)]))
    fold([(2, count - 2)], (0, tiles - 1))
    for c in z_sends:
        c.wait()
    inner.append(
        tally_up(
            [
                deferred(z, t, False, along_y, along_z)
                if t in (0, tiles - 1)
                else deferred(z, t, True, along_z)
                for z in outside
                for t in range(tiles)
            ]
        )
    )
    fold([(0, 2), (count - 2, count)], range(tiles))
    inner = functools.reduce(merge, inner)

    x_low.wait()
    x_high.wait()
    left_rim, right_rim = from_left[...], from_right[...]
    extra = (
        jnp.concatenate(
            [
                jnp.where(low_four, left_rim, pltpu.roll(right_rim, 4, 1)),
                jnp.where(low_four, pltpu.roll(left_rim, 124, 1), right_rim),
            ],
            axis=0,
        )
        - packed[...]
    )
    extra_hi = extra.astype(BF16)
    extra_lo = (extra - extra_hi.astype(F32)).astype(BF16)
    corr = jnp.dot(
        jnp.concatenate([extra_hi, extra_lo], axis=1), cross[...], preferred_element_type=F32
    ) * (1.0 / SCALE)
    rim = []
    for i in range(planes * tiles):
        at = slice(8 * i, 8 * i + 8)
        m = length(rim_slope[at, :] + corr[at], rim_square[at, :])
        rim_m[at, :] = m
        rim.append(classes(m, parity))
    rim = tally_up(rim)
    tally = acc[0] + acc[1]

    def only(keep, s):
        return (
            jnp.where(keep, s[0], 0.0),
            jnp.where(keep, s[1], 0.0),
            jnp.where(keep, s[2], 0.0),
            jnp.where(keep, s[3], BIG),
        )

    wsum, wcount, highest, lowest = functools.reduce(
        merge, [only(jnp.logical_not(outer), inner), rim]
    )

    keep = iota((GROUPS, WIDTH), 0) == lax.rem(iota((GROUPS, WIDTH), 1), GROUPS)

    def by_class(a):
        return jnp.sum(jnp.where(keep[None], a.reshape(COARSE, GROUPS, WIDTH), 0.0), axis=1)

    sums = jnp.concatenate([by_class(tally[0:SPAN, :]), by_class(tally[SPAN : 2 * SPAN, :])], axis=0)
    high = sums.astype(BF16)
    rest = sums - high.astype(F32)
    middle_bits = rest.astype(BF16)
    low_bits = (rest - middle_bits.astype(F32)).astype(BF16)
    three = jnp.dot(
        jnp.concatenate([high.astype(F32), middle_bits.astype(F32), low_bits.astype(F32)], axis=0).astype(BF16),
        unit[...],
        preferred_element_type=F32,
    )
    n = 2 * COARSE
    both = (three[2 * n : 3 * n] + three[n : 2 * n]) + three[0:n]
    place = iota((2 * COARSE, BINS), 1).astype(F32)
    digit = jnp.floor((place + 0.5) * (1.0 / FINE)).astype(jnp.int32)
    both = jnp.where(lax.rem(iota((2 * COARSE, BINS), 0), COARSE) == digit, both, 0.0)
    low_sum = jnp.sum(both[0:COARSE, :], axis=0, keepdims=True)
    part = jnp.sum(both[COARSE : 2 * COARSE, :], axis=0, keepdims=True)
    lane1 = iota((1, 128), 1)
    turned = [pltpu.roll(part[:, 0:128], 1, 1), pltpu.roll(part[:, 128:256], 1, 1)]
    row0 = low_sum[:, 0:128] - part[:, 0:128] + jnp.where(lane1 == 0, turned[1], turned[0])
    row1 = low_sum[:, 128:256] - part[:, 128:256] + jnp.where(lane1 == 0, turned[0], turned[1])

    def all_of(op, a):
        return op(op(a, axis=0, keepdims=True), axis=1, keepdims=True)

    row2 = jnp.where(
        lane1 == 0,
        all_of(jnp.min, lowest) + RANGE,
        jnp.where(
            lane1 == 1,
            all_of(jnp.max, highest),
            jnp.where(lane1 == 2, all_of(jnp.sum, wsum), all_of(jnp.sum, wcount)),
        ),
    )
    near = where["gx"] * sizes["gz"] + where["gz"]
    far = where["gy"]
    by_distance = lambda n: sorted(range(n), key=lambda d: -min(d, n - d))

    def share(buffer, slot, devices, i, meanwhile=lambda: None):
        for device in devices:
            pltpu.make_async_remote_copy(
                src_ref=buffer.at[slot],
                dst_ref=buffer.at[slot],
                send_sem=all_send.at[i],
                recv_sem=all_recv.at[i],
                device_id=device,
                device_id_type=MESH,
            ).start()
        others = buffer.at[pl.ds(0, len(devices))]
        arrival = pltpu.make_async_remote_copy(
            src_ref=others,
            dst_ref=others,
            send_sem=all_send.at[i],
            recv_sem=all_recv.at[i],
            device_id=up("gx"),
            device_id_type=MESH,
        )
        meanwhile()
        arrival.wait()
        parts = buffer[...]
        summed = jnp.sum(parts, axis=0)
        smallest = jnp.min(parts[:, 2:3], axis=0)
        largest = jnp.max(parts[:, 2:3], axis=0)
        stat = jnp.where(lane1 == 0, smallest, jnp.where(lane1 == 1, largest, summed[2:3]))
        return jnp.concatenate([summed[0:2], stat], axis=0)

    def put_rims():
        for i in range(planes * tiles):
            u, t = i // tiles, i % tiles
            m = rim_m[8 * i : 8 * i + 8, :]
            for j in range(count):
                at = (planes * j + u, slice(8 * t, 8 * t + 8), slice(None))
                mag_ref[at] = jnp.where(outer, back(m, j), mag_ref[at])

    gather_near[near] = jnp.concatenate([row0, row1, row2], axis=0)
    hear("gz", ready_z, 1)
    row = share(
        gather_near,
        near,
        [
            {"gx": ahead["gx", dx], "gz": ahead["gz", dz]}
            for dz in by_distance(sizes["gz"])
            for dx in by_distance(sizes["gx"])
            if dx or dz
        ],
        0,
        put_rims,
    )
    gather_far[far] = row
    hear("gy", ready_y, 1)
    row = share(gather_far, far, [{"gy": ahead["gy", dy]} for dy in by_distance(sizes["gy"]) if dy], 1)
    cells = nz * ny * nx * total
    hist_ref[...] = row[0:2] * (BINS / cells)
    stat_ref[...] = jnp.where(lane1 < 2, row[2:3], row[2:3] * (1.0 / cells))[:, 0:4]


def finish(*refs):
    results, outs, sems = refs[0:3], refs[3:6], refs[6]
    copies = [pltpu.make_async_copy(a, b, sems.at[i]) for i, (a, b) in enumerate(zip(results, outs))]
    for copy in copies:
        copy.start()
    for copy in copies:
        copy.wait()


def solution(mesh):
    sizes = dict(mesh.shape)

    def on_device(grid, first, beyond):
        nz, ny, nx = grid.shape
        vmem = pl.BlockSpec(memory_space=pltpu.VMEM)
        hbm = pl.BlockSpec(memory_space=pltpu.HBM)
        results = (
            jax.ShapeDtypeStruct(grid.shape, F32),
            jax.ShapeDtypeStruct((2, 128), F32),
            jax.ShapeDtypeStruct((1, 4), F32),
        )
        magnitude, histogram, stats = pl.pallas_call(
            functools.partial(kernel, sizes),
            out_shape=results,
            in_specs=[vmem, vmem, hbm],
            out_specs=(vmem, vmem, vmem),
            scratch_shapes=[
                pltpu.VMEM((nz + 8, ny + 16, nx), F32),
                pltpu.VMEM((2 * ny, 128), F32),
                pltpu.VMEM((ny, 128), F32),
                pltpu.VMEM((ny, 128), F32),
                pltpu.VMEM((ny, 128), F32),
                pltpu.VMEM((ny, 128), F32),
                pltpu.VMEM((nz, 4, nx), F32),
                pltpu.VMEM((nz, 4, nx), F32),
                pltpu.VMEM((nz, 4, nx), F32),
                pltpu.VMEM((nz, 4, nx), F32),
                pltpu.VMEM((256, 128), BF16),
                pltpu.VMEM((2 * ny, 128), F32),
                pltpu.VMEM((nz, ny, nx), F32),
                pltpu.VMEM((nz, ny, nx), F32),
                pltpu.VMEM((2 * ny, 128), F32),
                pltpu.VMEM((2 * ny, 128), F32),
                pltpu.VMEM((2, 2 * SPAN, WIDTH), F32),
                pltpu.VMEM((WIDTH, BINS), BF16),
                pltpu.VMEM((sizes["gx"] * sizes["gz"], 3, 128), F32),
                pltpu.VMEM((sizes["gy"], 3, 128), F32),
                pltpu.SemaphoreType.DMA((4,)),
                pltpu.SemaphoreType.DMA((6,)),
                pltpu.SemaphoreType.DMA((6,)),
                pltpu.SemaphoreType.REGULAR((2,)),
                pltpu.SemaphoreType.REGULAR((2,)),
                pltpu.SemaphoreType.DMA((2,)),
                pltpu.SemaphoreType.DMA((2,)),
            ],
            compiler_params=pltpu.CompilerParams(
                collective_id=0, has_side_effects=True, vmem_limit_bytes=VMEM_KIB * 1024
            ),
        )(first.reshape(1, 1), beyond.reshape(1, 1), pltpu.with_memory_space_constraint(grid, pltpu.HBM))
        magnitude, histogram, stats = pl.pallas_call(
            finish,
            out_shape=results,
            in_specs=[vmem, vmem, vmem],
            out_specs=(hbm, hbm, hbm),
            scratch_shapes=[pltpu.SemaphoreType.DMA((3,))],
            compiler_params=pltpu.CompilerParams(vmem_limit_bytes=4 * 1024 * 1024),
        )(magnitude, histogram, stats)
        return magnitude, histogram.reshape(BINS), stats.reshape(4)

    return jax.shard_map(
        on_device,
        mesh=mesh,
        in_specs=(P("gz", "gy", "gx"), P(), P()),
        out_specs=(P("gz", "gy", "gx"), P(), P()),
        check_vma=False,
    )
```

```python
import functools

import jax
import jax.numpy as jnp
from jax import lax
from jax.experimental import pallas as pl
from jax.experimental.pallas import tpu as pltpu
from jax.sharding import PartitionSpec as P

BINS = 256
FINE = 24
COARSE = 12
GROUPS = 8
RANGE = 12.0
COEFS = (0.8, -0.2, 4.0 / 105.0, -1.0 / 280.0)
SCALE = 840.0
TAPS = (672.0, -168.0, 32.0, -3.0)
MESH = pl.DeviceIdType.MESH
F32 = jnp.float32
BF16 = jnp.bfloat16
SPAN = COARSE * GROUPS
WIDTH = FINE * GROUPS
BIG = 3.0e38
VMEM_KIB = 32768
DOTS = 2
HALVES = 2


def tap(distance):
    value = jnp.zeros(distance.shape, F32)
    for k, t in enumerate(TAPS, start=1):
        value = jnp.where(distance == k, t, value)
        value = jnp.where(distance == -k, -t, value)
    return value


def iota(shape, axis):
    return lax.broadcasted_iota(jnp.int32, shape, axis)


def kernel(
    sizes,
    first_ref,
    beyond_ref,
    x_ref,
    mag_ref,
    hist_ref,
    stat_ref,
    ext,
    packed,
    to_right,
    to_left,
    from_left,
    from_right,
    to_above,
    to_below,
    from_below,
    from_above,
    cross,
    rim_m,
    slope,
    square,
    rim_slope,
    rim_square,
    acc,
    unit,
    gather_near,
    gather_far,
    in_sem,
    send_sem,
    recv_sem,
    ready_y,
    ready_z,
    all_send,
    all_recv,
):
    names = ("gx", "gy", "gz")
    nz, ny, nx = x_ref.shape
    tiles = ny // 8
    where = {a: lax.axis_index(a) for a in names}
    total = sizes["gx"] * sizes["gy"] * sizes["gz"]
    ahead = {(a, d): lax.rem(where[a] + d, sizes[a]) for a in names for d in range(sizes[a])}

    loads = [
        pltpu.make_async_copy(
            x_ref.at[pl.ds(a, b - a)], ext.at[pl.ds(4 + a, b - a), pl.ds(8, ny)], in_sem.at[i]
        )
        for i, (a, b) in enumerate(((0, 4), (nz - 4, nz), (4, nz // 2), (nz // 2, nz - 4)))
    ]
    for c in loads:
        c.start()

    def signal(sem, axis, distances):
        n = sizes[axis]
        steps = sorted({step % n for d in distances for step in (d, -d)} - {0})
        for d in steps:
            pl.semaphore_signal(sem, inc=1, device_id={axis: ahead[axis, d]}, device_id_type=MESH)
        return len(steps)

    barrier = pltpu.get_barrier_semaphore()
    greeted = (
        signal(barrier, "gx", range(1, sizes["gx"]))
        + signal(barrier, "gz", (1, 2))
        + signal(barrier, "gy", (1,))
    )
    z_hops = ((1, 2), range(3, sizes["gz"] // 2 + 1))
    y_hops = ((1,), (2,), (4,))
    heard = {}

    def tell(axis, sems, hops, i):
        heard[axis, i] = signal(sems.at[i], axis, hops[i])

    def hear(axis, sems, i):
        if heard[axis, i]:
            pl.semaphore_wait(sems.at[i], heard[axis, i])

    def up(a):
        return {a: ahead[a, 1]}

    def down(a):
        return {a: ahead[a, sizes[a] - 1]}

    def remote(src, dst, i, device):
        return pltpu.make_async_remote_copy(
            src_ref=src,
            dst_ref=dst,
            send_sem=send_sem.at[i],
            recv_sem=recv_sem.at[i],
            device_id=device,
            device_id_type=MESH,
        )

    own = slice(4, 4 + nz)
    wide = pl.ds(8, ny)

    def z_pair(low, high, i):
        return (
            remote(ext.at[pl.ds(nz + low, 2), wide], ext.at[pl.ds(low, 2), wide], i, up("gz")),
            remote(ext.at[pl.ds(high, 2), wide], ext.at[pl.ds(nz + high, 2), wide], i + 1, down("gz")),
        )

    z_near, z_far = z_pair(2, 4, 4), z_pair(0, 6, 6)
    y_low = remote(to_above, from_below, 2, up("gy"))
    y_high = remote(to_below, from_above, 3, down("gy"))
    x_low = remote(to_right, from_left, 0, up("gx"))
    x_high = remote(to_left, from_right, 1, down("gx"))

    planes = 2
    rows = planes * ny
    half = rows // 2
    lane = iota((8, 128), 1)
    outer = jnp.logical_or(lane < 4, lane >= nx - 4)
    low_four = lax.rem(iota((half, 128), 1), 8) < 4

    def turn(a, j):
        return pltpu.roll(a, (8 * j + 4) % 128, 1)

    def back(a, j):
        return pltpu.roll(a, (124 - 8 * j) % 128, 1)

    loads[0].wait()
    loads[1].wait()
    pl.semaphore_wait(barrier, greeted)
    for c in (*z_near, *z_far):
        c.start()
    loads[2].wait()
    loads[3].wait()
    to_above[...] = ext[own, 4 + ny : 8 + ny, :]
    to_below[...] = ext[own, 8:12, :]
    y_low.start()
    y_high.start()
    tell("gz", ready_z, z_hops, 0)
    tell("gy", ready_y, y_hops, 0)

    def second_difference(shift):
        from_step = iota((WIDTH, BINS), 0) // GROUPS
        bin_of = iota((WIDTH, BINS), 1) - shift
        digit = jnp.floor((bin_of.astype(F32) + 0.5) * (1.0 / FINE)).astype(jnp.int32)
        to_step = bin_of - FINE * digit
        single = jnp.where(to_step == FINE - 1, 1.0, 2.0)
        mix = jnp.where(from_step == to_step, single, jnp.where(jnp.abs(from_step - to_step) == 1, -1.0, 0.0))
        const = jnp.where(to_step == 0, 0.0, jnp.where(lax.rem(to_step, 2) == 1, -single, 2.0))
        return jnp.where(from_step == 0, const, mix).astype(BF16)

    r, c = iota((128, 128), 0), iota((128, 128), 1)
    same = jnp.logical_and(r // 8 == c // 8, (lax.rem(r, 8) < 4) != (lax.rem(c, 8) < 4))
    taps = jnp.where(same, tap(r - c), 0.0).astype(BF16)
    cross[...] = jnp.concatenate([taps, taps], axis=0)
    for i in range(2):
        unit[:, BINS * i : BINS * (i + 1)] = second_difference(i)

    lower = first_ref[...].astype(F32) - 1.0
    upper = beyond_ref[...].astype(F32)
    parity = jnp.where(iota((16, 128), 0) >= 8, 1.0, 0.0)
    lane16 = iota((16, 128), 1)
    never = jnp.full((16, 128), 1024.0, F32)
    inner_parity = jnp.where(jnp.logical_or(lane16 < 4, lane16 >= nx - 4), never, parity).astype(BF16)
    parity = parity.astype(BF16)
    zero = jnp.zeros((16, 128), BF16)
    one = jnp.ones((16, 128), BF16)

    def twice(a):
        return jnp.concatenate([a, a], axis=0).astype(BF16)

    def slant(pairs):
        total_ = None
        for c, (ahead_, behind) in zip(COEFS, pairs):
            term = ahead_ - behind
            total_ = term if total_ is None else total_ + (c / COEFS[0]) * term
        return total_

    steps = range(1, len(COEFS) + 1)

    def along_x(z, t):
        here = ext[z + 4, 8 + 8 * t : 16 + 8 * t, :]
        return slant([(pltpu.roll(here, 128 - k, 1), pltpu.roll(here, k, 1)) for k in steps])

    def along_y(z, t):
        y = 8 + 8 * t
        g = slant([(ext[z + 4, y + k : y + k + 8, :], ext[z + 4, y - k : y - k + 8, :]) for k in steps])
        return g * g

    def along_z(z, t):
        y = slice(8 + 8 * t, 16 + 8 * t)
        g = slant([(ext[z + 4 + k, y, :], ext[z + 4 - k, y, :]) for k in steps])
        return g * g

    def length(gx, rest):
        s = (rest + gx * gx) * COEFS[0] ** 2 + 1.0
        return s * lax.rsqrt(s) - 1.0

    def classes(m, offset):
        q = jnp.clip(m * (BINS / RANGE) - 0.5, 0.0, BINS - 1.0)
        low = jnp.minimum(jnp.floor(q), BINS - 2.0)
        w = jnp.clip(jnp.minimum(q - lower, upper - q), 0.0, 1.0)
        coarse = jnp.floor(low * (1.000001 / FINE))
        c2 = twice(coarse) - offset
        f2 = twice(low - FINE * coarse) - parity
        h2 = twice(q - low)
        ones, parts = [], []
        for j in range(COARSE // 2):
            hit = c2 == jnp.asarray(2 * j, BF16)
            ones.append(jnp.where(hit, one, zero))
            parts.append(jnp.where(hit, h2, zero))
        ladder = [jnp.minimum(f2, parity - one)]
        ladder += [jnp.minimum(f2, jnp.asarray(2 * j, BF16)) for j in range(1, FINE // 2)]
        wm = w * m
        stats = (wm, w, wm, m - RANGE * w)
        return jnp.concatenate(ones + parts, axis=0), jnp.concatenate(ladder, axis=0), stats

    def merge(a, b):
        return (a[0] + b[0], a[1] + b[1], jnp.maximum(a[2], b[2]), jnp.minimum(a[3], b[3]))

    def tally_up(items, fresh=False):
        share_of = len(items) // 2
        for i in range(2):
            part = items[i * share_of : (i + 1) * share_of]
            left = jnp.concatenate([a for a, _, _ in part], axis=1)
            right = jnp.concatenate([b for _, b, _ in part], axis=1)
            product = lax.dot_general(left, right, (((1,), (1,)), ((), ())), preferred_element_type=F32)
            if fresh:
                acc[i] = product
            else:
                acc[i] += product
        return functools.reduce(merge, [s for _, _, s in items])

    def place_of(z, t):
        return (z, slice(8 * t, 8 * t + 8), slice(None))

    def deferred(z, t, known=None, *parts):
        at = place_of(z, t)
        if known is None:
            gx, rest = along_x(z, t), None
            slope[at] = gx
        else:
            gx, rest = slope[at], square[at] if known else None
        for part in parts:
            g = part(z, t)
            rest = g if rest is None else rest + g
        square[at] = rest
        m = length(gx, rest)
        mag_ref[at] = m
        return classes(m, inner_parity)

    def prepare(z, t, part):
        at = place_of(z, t)
        slope[at] = along_x(z, t)
        if part is not None:
            square[at] = part(z, t)

    def fold(groups, span):
        for i in [u * tiles + t for u in range(planes) for t in span]:
            u, t = i // tiles, i % tiles
            for whole, kept in ((slope, rim_slope), (square, rim_square)):
                out = None
                for first, last in groups:
                    run = None
                    for j in range(first, last):
                        turned = turn(whole[planes * j + u, 8 * t : 8 * t + 8, :], j)
                        run = turned if run is None else jnp.where(lane >= 8 * j, turned, run)
                    if len(groups) == 1:
                        out = run
                    elif out is None:
                        out = jnp.where(lane < 8 * last, run, kept[8 * i : 8 * i + 8, :])
                    else:
                        out = jnp.where(lane >= 8 * first, run, out)
                kept[8 * i : 8 * i + 8, :] = out

    inside = list(range(4, nz - 4))
    count = nz // planes
    gathered = [None] * (planes * tiles)
    for i in range(planes * tiles):
        u, t = i // tiles, i % tiles
        for j in range(nz // planes):
            turned = turn(ext[4 + planes * j + u, 8 + 8 * t : 16 + 8 * t, :], j)
            gathered[i] = turned if j == 0 else jnp.where(lane >= 8 * j, turned, gathered[i])
        packed[8 * i : 8 * i + 8, :] = gathered[i]
    upper_half, lower_half = packed[0:half, :], packed[half:rows, :]
    to_right[...] = jnp.where(low_four, upper_half, pltpu.roll(lower_half, 4, 1))
    to_left[...] = jnp.where(low_four, pltpu.roll(upper_half, 124, 1), lower_half)
    x_low.start()
    x_high.start()
    outside = [z for z in range(nz) if z not in inside]
    for t in range(tiles):
        edge_row = t in (0, tiles - 1)
        for z in inside if edge_row else ():
            prepare(z, t, along_z)
        for z in outside:
            prepare(z, t, None if edge_row else along_y)
    inner = [
        tally_up([deferred(z, t, None, along_y, along_z) for z in inside for t in range(1, tiles - 1)], True)
    ]
    fold([(2, count - 2)], range(1, tiles - 1))

    hear("gz", ready_z, 0)
    hear("gy", ready_y, 0)
    tell("gz", ready_z, z_hops, 1)
    tell("gy", ready_y, y_hops, 1)
    y_low.wait()
    y_high.wait()
    ext[own, 4:8, :] = from_below[...]
    ext[own, 8 + ny : 12 + ny, :] = from_above[...]
    inner.append(tally_up([deferred(z, t, True, along_y) for z in inside for t in (0, tiles - 1)]))
    fold([(2, count - 2)], (0, tiles - 1))
    for sends, pair in ((z_near, (2, 3, nz - 4, nz - 3)), (z_far, (0, 1, nz - 2, nz - 1))):
        for c in sends:
            c.wait()
        inner.append(
            tally_up(
                [
                    deferred(z, t, False, along_y, along_z)
                    if t in (0, tiles - 1)
                    else deferred(z, t, True, along_z)
                    for z in pair
                    for t in range(tiles)
                ]
            )
        )
    fold([(0, 2), (count - 2, count)], range(tiles))
    inner = functools.reduce(merge, inner)

    hear("gy", ready_y, 1)
    tell("gy", ready_y, y_hops, 2)
    x_low.wait()
    x_high.wait()
    left_rim, right_rim = from_left[...], from_right[...]
    extra = (
        jnp.concatenate(
            [
                jnp.where(low_four, left_rim, pltpu.roll(right_rim, 4, 1)),
                jnp.where(low_four, pltpu.roll(left_rim, 124, 1), right_rim),
            ],
            axis=0,
        )
        - packed[...]
    )
    extra_hi = extra.astype(BF16)
    extra_lo = (extra - extra_hi.astype(F32)).astype(BF16)
    corr = jnp.dot(
        jnp.concatenate([extra_hi, extra_lo], axis=1), cross[...], preferred_element_type=F32
    ) * (1.0 / (SCALE * COEFS[0]))
    rim = []
    for i in range(planes * tiles):
        at = slice(8 * i, 8 * i + 8)
        m = length(rim_slope[at, :] + corr[at], rim_square[at, :])
        rim_m[at, :] = m
        rim.append(classes(m, parity))
    rim = tally_up(rim)
    tally = acc[0] + acc[1]

    def only(keep, s):
        return (
            jnp.where(keep, s[0], 0.0),
            jnp.where(keep, s[1], 0.0),
            jnp.where(keep, s[2], 0.0),
            jnp.where(keep, s[3], BIG),
        )

    wsum, wcount, highest, lowest = functools.reduce(
        merge, [only(jnp.logical_not(outer), inner), rim]
    )

    keep = iota((GROUPS, WIDTH), 0) == lax.rem(iota((GROUPS, WIDTH), 1), GROUPS)

    def by_class(a):
        return jnp.sum(jnp.where(keep[None], a.reshape(COARSE, GROUPS, WIDTH), 0.0), axis=1)

    parts = by_class(tally[SPAN : 2 * SPAN, :])
    sums = jnp.concatenate([by_class(tally[0:SPAN, :]) - parts, parts], axis=0)
    high = sums.astype(BF16).astype(F32)
    mid = (sums - high).astype(BF16).astype(F32)
    tail = sums - high - mid
    three = jnp.dot(
        jnp.concatenate([high, mid, tail], axis=0).astype(BF16), unit[...], preferred_element_type=F32
    )
    n = 2 * COARSE
    both = (three[2 * n : 3 * n] + three[n : 2 * n]) + three[0:n]
    class_of = iota((COARSE, BINS), 0)

    def at_home(shift):
        bins = (iota((COARSE, BINS), 1) - shift).astype(F32)
        return class_of == jnp.floor((bins + 0.5) * (1.0 / FINE)).astype(jnp.int32)

    bins = jnp.sum(
        jnp.where(at_home(0), both[0:COARSE, 0:BINS], 0.0)
        + jnp.where(at_home(1), both[COARSE:n, BINS : 2 * BINS], 0.0),
        axis=0,
        keepdims=True,
    )
    row0, row1 = bins[:, 0:128], bins[:, 128:256]
    lane1 = iota((1, 128), 1)

    def all_of(op, a):
        return op(op(a, axis=0, keepdims=True), axis=1, keepdims=True)

    row2 = jnp.where(
        lane1 == 0,
        all_of(jnp.min, lowest) + RANGE,
        jnp.where(
            lane1 == 1,
            all_of(jnp.max, highest),
            jnp.where(lane1 == 2, all_of(jnp.sum, wsum), all_of(jnp.sum, wcount)),
        ),
    )
    near = where["gx"] * sizes["gz"] + where["gz"]
    far = where["gy"]
    by_distance = lambda n: sorted(range(n), key=lambda d: -min(d, n - d))

    def share(buffer, slot, devices, i, meanwhile=lambda: None):
        for device in devices:
            pltpu.make_async_remote_copy(
                src_ref=buffer.at[slot],
                dst_ref=buffer.at[slot],
                send_sem=all_send.at[i],
                recv_sem=all_recv.at[i],
                device_id=device,
                device_id_type=MESH,
            ).start()
        others = buffer.at[pl.ds(0, len(devices))]
        arrival = pltpu.make_async_remote_copy(
            src_ref=others,
            dst_ref=others,
            send_sem=all_send.at[i],
            recv_sem=all_recv.at[i],
            device_id=up("gx"),
            device_id_type=MESH,
        )
        meanwhile()
        arrival.wait()
        parts = buffer[...]
        summed = jnp.sum(parts, axis=0)
        smallest = jnp.min(parts[:, 2:3], axis=0)
        largest = jnp.max(parts[:, 2:3], axis=0)
        stat = jnp.where(lane1 == 0, smallest, jnp.where(lane1 == 1, largest, summed[2:3]))
        return jnp.concatenate([summed[0:2], stat], axis=0)

    def put_rims():
        for i in range(planes * tiles):
            u, t = i // tiles, i % tiles
            m = rim_m[8 * i : 8 * i + 8, :]
            for j in range(count):
                at = (planes * j + u, slice(8 * t, 8 * t + 8), slice(None))
                mag_ref[at] = jnp.where(outer, back(m, j), mag_ref[at])

    gather_near[near] = jnp.concatenate([row0, row1, row2], axis=0)
    hear("gz", ready_z, 1)
    row = share(
        gather_near,
        near,
        [
            {"gx": ahead["gx", dx], "gz": ahead["gz", dz]}
            for dz in by_distance(sizes["gz"])
            for dx in by_distance(sizes["gx"])
            if dx or dz
        ],
        0,
        put_rims,
    )
    gather_far[far] = row
    hear("gy", ready_y, 2)
    row = share(gather_far, far, [{"gy": ahead["gy", dy]} for dy in by_distance(sizes["gy"]) if dy], 1)
    cells = nz * ny * nx * total
    hist_ref[...] = row[0:2] * (BINS / cells)
    stat_ref[...] = jnp.where(lane1 < 2, row[2:3], row[2:3] * (1.0 / cells))[:, 0:4]


def finish(*refs):
    results, outs, sems = refs[0:3], refs[3:6], refs[6]
    copies = [pltpu.make_async_copy(a, b, sems.at[i]) for i, (a, b) in enumerate(zip(results, outs))]
    for copy in copies:
        copy.start()
    for copy in copies:
        copy.wait()


def solution(mesh):
    sizes = dict(mesh.shape)

    def on_device(grid, first, beyond):
        nz, ny, nx = grid.shape
        vmem = pl.BlockSpec(memory_space=pltpu.VMEM)
        hbm = pl.BlockSpec(memory_space=pltpu.HBM)
        results = (
            jax.ShapeDtypeStruct(grid.shape, F32),
            jax.ShapeDtypeStruct((2, 128), F32),
            jax.ShapeDtypeStruct((1, 4), F32),
        )
        magnitude, histogram, stats = pl.pallas_call(
            functools.partial(kernel, sizes),
            out_shape=results,
            in_specs=[vmem, vmem, hbm],
            out_specs=(vmem, vmem, vmem),
            scratch_shapes=[
                pltpu.VMEM((nz + 8, ny + 16, nx), F32),
                pltpu.VMEM((2 * ny, 128), F32),
                pltpu.VMEM((ny, 128), F32),
                pltpu.VMEM((ny, 128), F32),
                pltpu.VMEM((ny, 128), F32),
                pltpu.VMEM((ny, 128), F32),
                pltpu.VMEM((nz, 4, nx), F32),
                pltpu.VMEM((nz, 4, nx), F32),
                pltpu.VMEM((nz, 4, nx), F32),
                pltpu.VMEM((nz, 4, nx), F32),
                pltpu.VMEM((256, 128), BF16),
                pltpu.VMEM((2 * ny, 128), F32),
                pltpu.VMEM((nz, ny, nx), F32),
                pltpu.VMEM((nz, ny, nx), F32),
                pltpu.VMEM((2 * ny, 128), F32),
                pltpu.VMEM((2 * ny, 128), F32),
                pltpu.VMEM((2, 2 * SPAN, WIDTH), F32),
                pltpu.VMEM((WIDTH, 2 * BINS), BF16),
                pltpu.VMEM((sizes["gx"] * sizes["gz"], 3, 128), F32),
                pltpu.VMEM((sizes["gy"], 3, 128), F32),
                pltpu.SemaphoreType.DMA((4,)),
                pltpu.SemaphoreType.DMA((8,)),
                pltpu.SemaphoreType.DMA((8,)),
                pltpu.SemaphoreType.REGULAR((3,)),
                pltpu.SemaphoreType.REGULAR((3,)),
                pltpu.SemaphoreType.DMA((2,)),
                pltpu.SemaphoreType.DMA((2,)),
            ],
            compiler_params=pltpu.CompilerParams(
                collective_id=0, has_side_effects=True, vmem_limit_bytes=VMEM_KIB * 1024
            ),
        )(first.reshape(1, 1), beyond.reshape(1, 1), pltpu.with_memory_space_constraint(grid, pltpu.HBM))
        magnitude, histogram, stats = pl.pallas_call(
            finish,
            out_shape=results,
            in_specs=[vmem, vmem, vmem],
            out_specs=(hbm, hbm, hbm),
            scratch_shapes=[pltpu.SemaphoreType.DMA((3,))],
            compiler_params=pltpu.CompilerParams(vmem_limit_bytes=4 * 1024 * 1024),
        )(magnitude, histogram, stats)
        return magnitude, histogram.reshape(BINS), stats.reshape(4)

    return jax.shard_map(
        on_device,
        mesh=mesh,
        in_specs=(P("gz", "gy", "gx"), P(), P()),
        out_specs=(P("gz", "gy", "gx"), P(), P()),
        check_vma=False,
    )
```

```python
import functools

import jax
import jax.numpy as jnp
from jax import lax
from jax.experimental import pallas as pl
from jax.experimental.pallas import tpu as pltpu
from jax.sharding import PartitionSpec as P

BINS = 256
FINE = 24
COARSE = 12
GROUPS = 8
RANGE = 12.0
COEFS = (0.8, -0.2, 4.0 / 105.0, -1.0 / 280.0)
SCALE = 840.0
TAPS = (672.0, -168.0, 32.0, -3.0)
MESH = pl.DeviceIdType.MESH
F32 = jnp.float32
BF16 = jnp.bfloat16
SPAN = COARSE * GROUPS
WIDTH = FINE * GROUPS
BIG = 3.0e38
VMEM_KIB = 32768
DOTS = 2
HALVES = 2


def tap(distance):
    value = jnp.zeros(distance.shape, F32)
    for k, t in enumerate(TAPS, start=1):
        value = jnp.where(distance == k, t, value)
        value = jnp.where(distance == -k, -t, value)
    return value


def iota(shape, axis):
    return lax.broadcasted_iota(jnp.int32, shape, axis)


def kernel(
    sizes,
    first_ref,
    beyond_ref,
    x_ref,
    mag_ref,
    hist_ref,
    stat_ref,
    ext,
    packed,
    to_right,
    to_left,
    from_left,
    from_right,
    to_above,
    to_below,
    from_below,
    from_above,
    cross,
    rim_m,
    slope,
    square,
    rim_slope,
    rim_square,
    acc,
    unit,
    gather_near,
    gather_far,
    in_sem,
    send_sem,
    recv_sem,
    ready_y,
    ready_z,
    all_send,
    all_recv,
):
    names = ("gx", "gy", "gz")
    nz, ny, nx = x_ref.shape
    tiles = ny // 8
    where = {a: lax.axis_index(a) for a in names}
    total = sizes["gx"] * sizes["gy"] * sizes["gz"]
    ahead = {(a, d): lax.rem(where[a] + d, sizes[a]) for a in names for d in range(sizes[a])}

    loads = [
        pltpu.make_async_copy(
            x_ref.at[pl.ds(a, b - a)], ext.at[pl.ds(4 + a, b - a), pl.ds(8, ny)], in_sem.at[i]
        )
        for i, (a, b) in enumerate(((0, 4), (nz - 4, nz), (4, nz // 2), (nz // 2, nz - 4)))
    ]
    for c in loads:
        c.start()

    def signal(sem, axis, distances):
        n = sizes[axis]
        steps = sorted({step % n for d in distances for step in (d, -d)} - {0})
        for d in steps:
            pl.semaphore_signal(sem, inc=1, device_id={axis: ahead[axis, d]}, device_id_type=MESH)
        return len(steps)

    barrier = pltpu.get_barrier_semaphore()
    greeted = (
        signal(barrier, "gx", range(1, sizes["gx"]))
        + signal(barrier, "gz", (1, 2))
        + signal(barrier, "gy", (1,))
    )
    z_hops = ((1, 2), range(3, sizes["gz"] // 2 + 1))
    y_hops = ((1,), (2,), (4,))
    heard = {}

    def tell(axis, sems, hops, i):
        heard[axis, i] = signal(sems.at[i], axis, hops[i])

    def hear(axis, sems, i):
        if heard[axis, i]:
            pl.semaphore_wait(sems.at[i], heard[axis, i])

    def up(a):
        return {a: ahead[a, 1]}

    def down(a):
        return {a: ahead[a, sizes[a] - 1]}

    def remote(src, dst, i, device):
        return pltpu.make_async_remote_copy(
            src_ref=src,
            dst_ref=dst,
            send_sem=send_sem.at[i],
            recv_sem=recv_sem.at[i],
            device_id=device,
            device_id_type=MESH,
        )

    own = slice(4, 4 + nz)
    wide = pl.ds(8, ny)

    def z_pair(low, high, i):
        return (
            remote(ext.at[pl.ds(nz + low, 2), wide], ext.at[pl.ds(low, 2), wide], i, up("gz")),
            remote(ext.at[pl.ds(high, 2), wide], ext.at[pl.ds(nz + high, 2), wide], i + 1, down("gz")),
        )

    z_near, z_far = z_pair(2, 4, 4), z_pair(0, 6, 6)
    y_low = remote(to_above, from_below, 2, up("gy"))
    y_high = remote(to_below, from_above, 3, down("gy"))
    x_low = remote(to_right, from_left, 0, up("gx"))
    x_high = remote(to_left, from_right, 1, down("gx"))

    planes = 2
    rows = planes * ny
    half = rows // 2
    lane = iota((8, 128), 1)
    outer = jnp.logical_or(lane < 4, lane >= nx - 4)
    low_four = lax.rem(iota((half, 128), 1), 8) < 4

    def turn(a, j):
        return pltpu.roll(a, (8 * j + 4) % 128, 1)

    def back(a, j):
        return pltpu.roll(a, (124 - 8 * j) % 128, 1)

    loads[0].wait()
    loads[1].wait()
    pl.semaphore_wait(barrier, greeted)
    for c in z_near:
        c.start()
    loads[2].wait()
    loads[3].wait()
    to_above[...] = ext[own, 4 + ny : 8 + ny, :]
    to_below[...] = ext[own, 8:12, :]
    y_low.start()
    y_high.start()
    tell("gz", ready_z, z_hops, 0)
    tell("gy", ready_y, y_hops, 0)

    def second_difference(shift):
        from_step = iota((WIDTH, BINS), 0) // GROUPS
        bin_of = iota((WIDTH, BINS), 1) - shift
        digit = jnp.floor((bin_of.astype(F32) + 0.5) * (1.0 / FINE)).astype(jnp.int32)
        to_step = bin_of - FINE * digit
        single = jnp.where(to_step == FINE - 1, 1.0, 2.0)
        mix = jnp.where(from_step == to_step, single, jnp.where(jnp.abs(from_step - to_step) == 1, -1.0, 0.0))
        const = jnp.where(to_step == 0, 0.0, jnp.where(lax.rem(to_step, 2) == 1, -single, 2.0))
        return jnp.where(from_step == 0, const, mix).astype(BF16)

    r, c = iota((128, 128), 0), iota((128, 128), 1)
    same = jnp.logical_and(r // 8 == c // 8, (lax.rem(r, 8) < 4) != (lax.rem(c, 8) < 4))
    taps = jnp.where(same, tap(r - c), 0.0).astype(BF16)
    cross[...] = jnp.concatenate([taps, taps], axis=0)
    for i in range(2):
        unit[:, BINS * i : BINS * (i + 1)] = second_difference(i)

    lower = first_ref[...].astype(F32) - 1.0
    upper = beyond_ref[...].astype(F32)
    parity = jnp.where(iota((16, 128), 0) >= 8, 1.0, 0.0)
    lane16 = iota((16, 128), 1)
    never = jnp.full((16, 128), 1024.0, F32)
    inner_parity = jnp.where(jnp.logical_or(lane16 < 4, lane16 >= nx - 4), never, parity).astype(BF16)
    parity = parity.astype(BF16)
    zero = jnp.zeros((16, 128), BF16)
    one = jnp.ones((16, 128), BF16)

    def twice(a):
        return jnp.concatenate([a, a], axis=0).astype(BF16)

    def slant(pairs):
        total_ = None
        for c, (ahead_, behind) in zip(COEFS, pairs):
            term = ahead_ - behind
            total_ = term if total_ is None else total_ + (c / COEFS[0]) * term
        return total_

    steps = range(1, len(COEFS) + 1)

    def along_x(z, t):
        here = ext[z + 4, 8 + 8 * t : 16 + 8 * t, :]
        return slant([(pltpu.roll(here, 128 - k, 1), pltpu.roll(here, k, 1)) for k in steps])

    def along_y(z, t):
        y = 8 + 8 * t
        g = slant([(ext[z + 4, y + k : y + k + 8, :], ext[z + 4, y - k : y - k + 8, :]) for k in steps])
        return g * g

    def along_z(z, t):
        y = slice(8 + 8 * t, 16 + 8 * t)
        g = slant([(ext[z + 4 + k, y, :], ext[z + 4 - k, y, :]) for k in steps])
        return g * g

    def length(gx, rest):
        s = (rest + gx * gx) * COEFS[0] ** 2 + 1.0
        return s * lax.rsqrt(s) - 1.0

    def classes(m, offset):
        q = jnp.clip(m * (BINS / RANGE) - 0.5, 0.0, BINS - 1.0)
        low = jnp.minimum(jnp.floor(q), BINS - 2.0)
        w = jnp.clip(jnp.minimum(q - lower, upper - q), 0.0, 1.0)
        coarse = jnp.floor(low * (1.000001 / FINE))
        c2 = twice(coarse) - offset
        f2 = twice(low - FINE * coarse) - parity
        h2 = twice(q - low)
        ones, parts = [], []
        for j in range(COARSE // 2):
            hit = c2 == jnp.asarray(2 * j, BF16)
            ones.append(jnp.where(hit, one, zero))
            parts.append(jnp.where(hit, h2, zero))
        ladder = [jnp.minimum(f2, parity - one)]
        ladder += [jnp.minimum(f2, jnp.asarray(2 * j, BF16)) for j in range(1, FINE // 2)]
        wm = w * m
        stats = (wm, w, wm, m - RANGE * w)
        return jnp.concatenate(ones + parts, axis=0), jnp.concatenate(ladder, axis=0), stats

    def merge(a, b):
        return (a[0] + b[0], a[1] + b[1], jnp.maximum(a[2], b[2]), jnp.minimum(a[3], b[3]))

    def tally_up(items, fresh=False):
        share_of = len(items) // 2
        for i in range(2):
            part = items[i * share_of : (i + 1) * share_of]
            left = jnp.concatenate([a for a, _, _ in part], axis=1)
            right = jnp.concatenate([b for _, b, _ in part], axis=1)
            product = lax.dot_general(left, right, (((1,), (1,)), ((), ())), preferred_element_type=F32)
            if fresh:
                acc[i] = product
            else:
                acc[i] += product
        return functools.reduce(merge, [s for _, _, s in items])

    def place_of(z, t):
        return (z, slice(8 * t, 8 * t + 8), slice(None))

    def deferred(z, t, known=None, *parts):
        at = place_of(z, t)
        if known is None:
            gx, rest = along_x(z, t), None
            slope[at] = gx
        else:
            gx, rest = slope[at], square[at] if known else None
        for part in parts:
            g = part(z, t)
            rest = g if rest is None else rest + g
        square[at] = rest
        m = length(gx, rest)
        mag_ref[at] = m
        return classes(m, inner_parity)

    def prepare(z, t, part):
        at = place_of(z, t)
        slope[at] = along_x(z, t)
        if part is not None:
            square[at] = part(z, t)

    def fold(groups, span):
        for i in [u * tiles + t for u in range(planes) for t in span]:
            u, t = i // tiles, i % tiles
            for whole, kept in ((slope, rim_slope), (square, rim_square)):
                out = None
                for first, last in groups:
                    run = None
                    for j in range(first, last):
                        turned = turn(whole[planes * j + u, 8 * t : 8 * t + 8, :], j)
                        run = turned if run is None else jnp.where(lane >= 8 * j, turned, run)
                    if len(groups) == 1:
                        out = run
                    elif out is None:
                        out = jnp.where(lane < 8 * last, run, kept[8 * i : 8 * i + 8, :])
                    else:
                        out = jnp.where(lane >= 8 * first, run, out)
                kept[8 * i : 8 * i + 8, :] = out

    inside = list(range(4, nz - 4))
    count = nz // planes
    gathered = [None] * (planes * tiles)
    for i in range(planes * tiles):
        u, t = i // tiles, i % tiles
        for j in range(nz // planes):
            turned = turn(ext[4 + planes * j + u, 8 + 8 * t : 16 + 8 * t, :], j)
            gathered[i] = turned if j == 0 else jnp.where(lane >= 8 * j, turned, gathered[i])
        packed[8 * i : 8 * i + 8, :] = gathered[i]
    upper_half, lower_half = packed[0:half, :], packed[half:rows, :]
    to_right[...] = jnp.where(low_four, upper_half, pltpu.roll(lower_half, 4, 1))
    to_left[...] = jnp.where(low_four, pltpu.roll(upper_half, 124, 1), lower_half)
    for c in (x_low, x_high, *z_far):
        c.start()
    outside = [z for z in range(nz) if z not in inside]
    for t in range(tiles):
        edge_row = t in (0, tiles - 1)
        for z in inside if edge_row else ():
            prepare(z, t, along_z)
        for z in outside:
            prepare(z, t, None if edge_row else along_y)
    inner = [
        tally_up([deferred(z, t, None, along_y, along_z) for z in inside for t in range(1, tiles - 1)], True)
    ]
    fold([(2, count - 2)], range(1, tiles - 1))

    hear("gz", ready_z, 0)
    hear("gy", ready_y, 0)
    tell("gz", ready_z, z_hops, 1)
    tell("gy", ready_y, y_hops, 1)
    y_low.wait()
    y_high.wait()
    ext[own, 4:8, :] = from_below[...]
    ext[own, 8 + ny : 12 + ny, :] = from_above[...]
    inner.append(tally_up([deferred(z, t, True, along_y) for z in inside for t in (0, tiles - 1)]))
    fold([(2, count - 2)], (0, tiles - 1))
    for sends, pair in ((z_near, (2, 3, nz - 4, nz - 3)), (z_far, (0, 1, nz - 2, nz - 1))):
        for c in sends:
            c.wait()
        inner.append(
            tally_up(
                [
                    deferred(z, t, False, along_y, along_z)
                    if t in (0, tiles - 1)
                    else deferred(z, t, True, along_z)
                    for z in pair
                    for t in range(tiles)
                ]
            )
        )
    fold([(0, 2), (count - 2, count)], range(tiles))
    inner = functools.reduce(merge, inner)

    hear("gy", ready_y, 1)
    tell("gy", ready_y, y_hops, 2)
    x_low.wait()
    x_high.wait()
    left_rim, right_rim = from_left[...], from_right[...]
    extra = (
        jnp.concatenate(
            [
                jnp.where(low_four, left_rim, pltpu.roll(right_rim, 4, 1)),
                jnp.where(low_four, pltpu.roll(left_rim, 124, 1), right_rim),
            ],
            axis=0,
        )
        - packed[...]
    )
    extra_hi = extra.astype(BF16)
    extra_lo = (extra - extra_hi.astype(F32)).astype(BF16)
    corr = jnp.dot(
        jnp.concatenate([extra_hi, extra_lo], axis=1), cross[...], preferred_element_type=F32
    ) * (1.0 / (SCALE * COEFS[0]))
    rim = []
    for i in range(planes * tiles):
        at = slice(8 * i, 8 * i + 8)
        m = length(rim_slope[at, :] + corr[at], rim_square[at, :])
        rim_m[at, :] = m
        rim.append(classes(m, parity))
    rim = tally_up(rim)
    tally = acc[0] + acc[1]

    def only(keep, s):
        return (
            jnp.where(keep, s[0], 0.0),
            jnp.where(keep, s[1], 0.0),
            jnp.where(keep, s[2], 0.0),
            jnp.where(keep, s[3], BIG),
        )

    wsum, wcount, highest, lowest = functools.reduce(
        merge, [only(jnp.logical_not(outer), inner), rim]
    )

    keep = iota((GROUPS, WIDTH), 0) == lax.rem(iota((GROUPS, WIDTH), 1), GROUPS)

    def by_class(a):
        return jnp.sum(jnp.where(keep[None], a.reshape(COARSE, GROUPS, WIDTH), 0.0), axis=1)

    parts = by_class(tally[SPAN : 2 * SPAN, :])
    sums = jnp.concatenate([by_class(tally[0:SPAN, :]) - parts, parts], axis=0)
    high = sums.astype(BF16).astype(F32)
    mid = (sums - high).astype(BF16).astype(F32)
    tail = sums - high - mid
    three = jnp.dot(
        jnp.concatenate([high, mid, tail], axis=0).astype(BF16), unit[...], preferred_element_type=F32
    )
    n = 2 * COARSE
    both = (three[2 * n : 3 * n] + three[n : 2 * n]) + three[0:n]
    class_of = iota((COARSE, BINS), 0)

    def at_home(shift):
        bins = (iota((COARSE, BINS), 1) - shift).astype(F32)
        return class_of == jnp.floor((bins + 0.5) * (1.0 / FINE)).astype(jnp.int32)

    bins = jnp.sum(
        jnp.where(at_home(0), both[0:COARSE, 0:BINS], 0.0)
        + jnp.where(at_home(1), both[COARSE:n, BINS : 2 * BINS], 0.0),
        axis=0,
        keepdims=True,
    )
    row0, row1 = bins[:, 0:128], bins[:, 128:256]
    lane1 = iota((1, 128), 1)

    def all_of(op, a):
        return op(op(a, axis=0, keepdims=True), axis=1, keepdims=True)

    row2 = jnp.where(
        lane1 == 0,
        all_of(jnp.min, lowest) + RANGE,
        jnp.where(
            lane1 == 1,
            all_of(jnp.max, highest),
            jnp.where(lane1 == 2, all_of(jnp.sum, wsum), all_of(jnp.sum, wcount)),
        ),
    )
    near = where["gx"] * sizes["gz"] + where["gz"]
    far = where["gy"]
    by_distance = lambda n: sorted(range(n), key=lambda d: -min(d, n - d))

    def share(buffer, slot, devices, i, meanwhile=lambda: None):
        for device in devices:
            pltpu.make_async_remote_copy(
                src_ref=buffer.at[slot],
                dst_ref=buffer.at[slot],
                send_sem=all_send.at[i],
                recv_sem=all_recv.at[i],
                device_id=device,
                device_id_type=MESH,
            ).start()
        others = buffer.at[pl.ds(0, len(devices))]
        arrival = pltpu.make_async_remote_copy(
            src_ref=others,
            dst_ref=others,
            send_sem=all_send.at[i],
            recv_sem=all_recv.at[i],
            device_id=up("gx"),
            device_id_type=MESH,
        )
        meanwhile()
        arrival.wait()
        parts = buffer[...]
        summed = jnp.sum(parts, axis=0)
        smallest = jnp.min(parts[:, 2:3], axis=0)
        largest = jnp.max(parts[:, 2:3], axis=0)
        stat = jnp.where(lane1 == 0, smallest, jnp.where(lane1 == 1, largest, summed[2:3]))
        return jnp.concatenate([summed[0:2], stat], axis=0)

    def put_rims():
        for i in range(planes * tiles):
            u, t = i // tiles, i % tiles
            m = rim_m[8 * i : 8 * i + 8, :]
            for j in range(count):
                at = (planes * j + u, slice(8 * t, 8 * t + 8), slice(None))
                mag_ref[at] = jnp.where(outer, back(m, j), mag_ref[at])

    gather_near[near] = jnp.concatenate([row0, row1, row2], axis=0)
    hear("gz", ready_z, 1)
    row = share(
        gather_near,
        near,
        [
            {"gx": ahead["gx", dx], "gz": ahead["gz", dz]}
            for dz in by_distance(sizes["gz"])
            for dx in by_distance(sizes["gx"])
            if dx or dz
        ],
        0,
        put_rims,
    )
    gather_far[far] = row
    hear("gy", ready_y, 2)
    row = share(gather_far, far, [{"gy": ahead["gy", dy]} for dy in by_distance(sizes["gy"]) if dy], 1)
    cells = nz * ny * nx * total
    hist_ref[...] = row[0:2] * (BINS / cells)
    stat_ref[...] = jnp.where(lane1 < 2, row[2:3], row[2:3] * (1.0 / cells))[:, 0:4]


def finish(*refs):
    results, outs, sems = refs[0:3], refs[3:6], refs[6]
    copies = [pltpu.make_async_copy(a, b, sems.at[i]) for i, (a, b) in enumerate(zip(results, outs))]
    for copy in copies:
        copy.start()
    for copy in copies:
        copy.wait()


def solution(mesh):
    sizes = dict(mesh.shape)

    def on_device(grid, first, beyond):
        nz, ny, nx = grid.shape
        vmem = pl.BlockSpec(memory_space=pltpu.VMEM)
        hbm = pl.BlockSpec(memory_space=pltpu.HBM)
        results = (
            jax.ShapeDtypeStruct(grid.shape, F32),
            jax.ShapeDtypeStruct((2, 128), F32),
            jax.ShapeDtypeStruct((1, 4), F32),
        )
        magnitude, histogram, stats = pl.pallas_call(
            functools.partial(kernel, sizes),
            out_shape=results,
            in_specs=[vmem, vmem, hbm],
            out_specs=(vmem, vmem, vmem),
            scratch_shapes=[
                pltpu.VMEM((nz + 8, ny + 16, nx), F32),
                pltpu.VMEM((2 * ny, 128), F32),
                pltpu.VMEM((ny, 128), F32),
                pltpu.VMEM((ny, 128), F32),
                pltpu.VMEM((ny, 128), F32),
                pltpu.VMEM((ny, 128), F32),
                pltpu.VMEM((nz, 4, nx), F32),
                pltpu.VMEM((nz, 4, nx), F32),
                pltpu.VMEM((nz, 4, nx), F32),
                pltpu.VMEM((nz, 4, nx), F32),
                pltpu.VMEM((256, 128), BF16),
                pltpu.VMEM((2 * ny, 128), F32),
                pltpu.VMEM((nz, ny, nx), F32),
                pltpu.VMEM((nz, ny, nx), F32),
                pltpu.VMEM((2 * ny, 128), F32),
                pltpu.VMEM((2 * ny, 128), F32),
                pltpu.VMEM((2, 2 * SPAN, WIDTH), F32),
                pltpu.VMEM((WIDTH, 2 * BINS), BF16),
                pltpu.VMEM((sizes["gx"] * sizes["gz"], 3, 128), F32),
                pltpu.VMEM((sizes["gy"], 3, 128), F32),
                pltpu.SemaphoreType.DMA((4,)),
                pltpu.SemaphoreType.DMA((8,)),
                pltpu.SemaphoreType.DMA((8,)),
                pltpu.SemaphoreType.REGULAR((3,)),
                pltpu.SemaphoreType.REGULAR((3,)),
                pltpu.SemaphoreType.DMA((2,)),
                pltpu.SemaphoreType.DMA((2,)),
            ],
            compiler_params=pltpu.CompilerParams(
                collective_id=0,
                has_side_effects=True,
                vmem_limit_bytes=VMEM_KIB * 1024
            ),
        )(first.reshape(1, 1), beyond.reshape(1, 1), pltpu.with_memory_space_constraint(grid, pltpu.HBM))
        magnitude, histogram, stats = pl.pallas_call(
            finish,
            out_shape=results,
            in_specs=[vmem, vmem, vmem],
            out_specs=(hbm, hbm, hbm),
            scratch_shapes=[pltpu.SemaphoreType.DMA((3,))],
            compiler_params=pltpu.CompilerParams(vmem_limit_bytes=4 * 1024 * 1024),
        )(magnitude, histogram, stats)
        return magnitude, histogram.reshape(BINS), stats.reshape(4)

    return jax.shard_map(
        on_device,
        mesh=mesh,
        in_specs=(P("gz", "gy", "gx"), P(), P()),
        out_specs=(P("gz", "gy", "gx"), P(), P()),
        check_vma=False,
    )
```
